32 devices in a mesh: obs: 8 (over z, x), bel: 4 (over y, core).
Axes of the slice: x: 2, y: 2, z: 4, core: 2. Of those that a mesh axis runs over, the one named last changes fastest.
Arguments:
- alpha_set: bfloat16 [2048, 2048], P('bel'), may hold values from -600 to 600
- transitions: bfloat16 [16, 2048, 2048], P(None, 'obs'), may hold values from 0.0009994507 to 1
- obs_weights: float32 [256, 16, 2048], P('obs'), may hold values from 0.01 to 1
- rewards: float32 [16, 2048], replicated, may hold values from -1 to 1
- chosen_idx: int32 [1536, 16, 256], P('bel', None, 'obs'), may hold values from 0 to 2047
- chosen_action: int32 [1536], P('bel'), may hold values from 0 to 15
Outputs:
- new_alpha: float32 [1536, 2048], P(('bel', 'obs'))
The draws below stay inside these ranges and needn't reach their ends.
Inputs may be any that keep to these rules, and one draw needn't show every extreme that they name: `chosen_idx`: an index into the 2048 alpha vectors. `chosen_action`: an index into the 16 actions.
All inputs are finite; a program needn't handle non-finite values.
Results may differ from the reference program's by a relative error of at most 0.0003.
Values may be sent and summed in bfloat16 or wider, within the bound.
A program may use at most 192 MiB of HBM per device.

```python
import math
import jax
import jax.numpy as jnp
from jax import lax

S = 2048
A = 16
O = 256
K = 2048
BEL = 1536


def touch_ends(result, stream_key, low, largest):
    spot = [jax.random.randint(jax.random.fold_in(stream_key, axis), (), 0, length) for axis, length in enumerate(result.shape)]
    widest = result.shape.index(max(result.shape))
    next_to = spot[:widest] + [(spot[widest] + 1) % result.shape[widest]] + spot[widest + 1:]
    return result.at[tuple(spot)].set(low).at[tuple(next_to)].set(largest)


def levels(stream_key, shape, pieces, smallest, top_value):
    def one(axis_at, blocks):
        draws = jax.random.uniform(jax.random.fold_in(jax.random.fold_in(stream_key, 6), axis_at), (blocks,), jnp.float32, smallest / len(pieces), top_value / len(pieces))
        return jnp.repeat(jnp.exp(draws), shape[axis_at] // blocks).reshape((-1,) + (1,) * (len(shape) - axis_at - 1))

    gain = one(*pieces[0])
    for cut in pieces[1:]:
        gain = gain * one(*cut)
    return gain


def bell_draw(key, dims, spread, most, split=(), kind=jnp.bfloat16):
    gain = levels(key, dims, split, -0.22, 0.18) if split else 1.0
    array = jax.random.normal(key, dims, jnp.float32) * spread * gain
    return jnp.minimum(jnp.maximum(array, -most), most).astype(kind)


def setup_inputs(seed: int = 0) -> dict:
    streams_of = jax.random.split(jax.random.key(seed), 7)
    alpha_set = bell_draw(streams_of[0], (K, S), 100.0, 600.0, ((0, 4),))
    transitions = jnp.clip(jnp.exp(math.log(1.0) - 6.9083047 * jax.random.uniform(streams_of[1], (A, S, S), jnp.float32) ** levels(streams_of[1], (A, S, S), ((1, 8),), -0.2, 0.2)), 0.0009994507, 1.0).astype(jnp.bfloat16)
    obs_weights = jnp.clip(jnp.exp(math.log(1.0) - 4.6051702 * jax.random.uniform(streams_of[2], (O, A, S), jnp.float32) ** levels(streams_of[2], (O, A, S), ((0, 8),), -0.2, 0.2)), 0.01, 1.0)
    rewards = jnp.clip(jax.random.uniform(streams_of[3], (A, S), jnp.float32, -1.0, 1.0), -1.0, 1.0)
    chosen_idx = touch_ends(jax.random.randint(streams_of[4], (BEL, A, O), 0, K), jax.random.fold_in(streams_of[4], 1), 0, K - 1).astype(jnp.int32)
    chosen_action = touch_ends(jax.random.randint(streams_of[5], (BEL,), 0, A), jax.random.fold_in(streams_of[5], 1), 0, A - 1).astype(jnp.int32)
    return {"alpha_set": alpha_set, "transitions": transitions, "obs_weights": obs_weights, "rewards": rewards, "chosen_idx": chosen_idx, "chosen_action": chosen_action}


discount = 0.95


def reference(alpha_set, transitions, obs_weights, rewards, chosen_idx, chosen_action):
    obs_prob = obs_weights / jnp.sum(obs_weights, axis=0, keepdims=True)
    trans_raw = transitions.astype(jnp.float32)
    trans_prob = trans_raw / jnp.sum(trans_raw, axis=1, keepdims=True)
    picked = jnp.take_along_axis(chosen_idx, chosen_action[:, None, None], axis=1)[:, 0, :]

    def add_obs(total, index):
        rows = jnp.take(alpha_set, picked[:, index], axis=0).astype(jnp.float32)
        probs = jnp.take(obs_prob[index], chosen_action, axis=0)
        return total + probs * rows, None

    start = jnp.zeros((BEL, S), jnp.float32)
    weighted, _ = lax.scan(add_obs, start, jnp.arange(O, dtype=jnp.int32))
    action_hot = (chosen_action[:, None] == jnp.arange(A, dtype=jnp.int32)[None, :]).astype(jnp.float32)

    def add_action(total, index):
        block = lax.dynamic_index_in_dim(trans_prob, index, 0, keepdims=False)
        moved = jnp.dot(weighted, block, precision=lax.Precision.HIGHEST, preferred_element_type=jnp.float32)
        column = lax.dynamic_slice_in_dim(action_hot, index, 1, 1)
        return total + column * moved, None

    future, _ = lax.scan(add_action, jnp.zeros((BEL, S), jnp.float32), jnp.arange(A, dtype=jnp.int32))
    reward_rows = jnp.take(rewards, chosen_action, axis=0)
    return reward_rows + discount * future
```

```python
import functools

import jax
import jax.numpy as jnp
from jax import lax
from jax.experimental import pallas as pl
from jax.experimental.pallas import tpu as pltpu
from jax.sharding import PartitionSpec as P

discount = 0.95
lanes = 128


def gather_kernel(picks_ref, act_ref, alpha_ref, weights_ref, moves_ref, out_ref):
    beliefs = act_ref.shape[0]
    obs_local = picks_ref.shape[0] // beliefs
    actions = weights_ref.shape[0] // obs_local
    slabs = alpha_ref.shape[1]
    rows = out_ref.shape[0] // slabs

    def one(b, carry):
        action = act_ref[b]
        sums = [None] * min(4, obs_local)
        for o in range(obs_local):
            row = alpha_ref[picks_ref[b * obs_local + o]].astype(jnp.float32)
            term = row * weights_ref[o * actions + action]
            at = o % len(sums)
            sums[at] = term if sums[at] is None else sums[at] + term
        out_ref[pl.ds(b, slabs, stride=rows), :] = functools.reduce(jnp.add, sums)
        return carry

    lax.fori_loop(0, beliefs, one, 0)

    def total(a, carry):
        acc = weights_ref[a]
        for o in range(1, obs_local):
            acc = acc + weights_ref[o * actions + a]
        out_ref[pl.ds(beliefs + a, slabs, stride=rows), :] = acc
        out_ref[pl.ds(beliefs + actions + a, slabs, stride=rows), :] = moves_ref[a]
        return carry

    lax.fori_loop(0, actions, total, 0)


def gather_rows(picks, acts, alpha, weights, moves):
    slabs = alpha.shape[1]
    beliefs = acts.shape[0]
    rows = beliefs + 2 * moves.shape[0]
    vmem = pl.BlockSpec(memory_space=pltpu.VMEM)
    smem = pl.BlockSpec(memory_space=pltpu.SMEM)
    out = pl.pallas_call(
        gather_kernel,
        out_shape=jax.ShapeDtypeStruct((slabs * rows, lanes), jnp.float32),
        in_specs=[smem, smem, vmem, vmem, vmem],
        out_specs=vmem,
        compiler_params=pltpu.CompilerParams(vmem_limit_bytes=40 << 20),
        cost_estimate=pl.CostEstimate(
            flops=80_000_000, bytes_accessed=16 << 20, transcendentals=0
        ),
        name="gather_rows",
    )(picks, acts, alpha, weights, moves)
    return out.reshape(slabs, rows, lanes)


def move_kernel(act_ref, w_ref, tot_ref, table_ref, out_ref):
    a = pl.program_id(0)
    scaled = w_ref[...] / tot_ref[0]
    x = jnp.where(act_ref[...] == a, scaled, 0.0)
    high = x.astype(jnp.bfloat16)
    low = (x - high.astype(jnp.float32)).astype(jnp.bfloat16)
    table = table_ref[0]
    both = jnp.dot(jnp.concatenate([high, low], axis=0), table, preferred_element_type=jnp.float32)
    half = x.shape[0]
    part = both[:half] + both[half:]

    @pl.when(a == 0)
    def _():
        out_ref[...] = part

    @pl.when(a > 0)
    def _():
        out_ref[...] += part


def move(acts, weighted, totals, table):
    beliefs, width = weighted.shape
    actions, _, states = table.shape
    return pl.pallas_call(
        move_kernel,
        grid=(actions,),
        out_shape=jax.ShapeDtypeStruct((beliefs, states), jnp.float32),
        in_specs=[
            pl.BlockSpec((beliefs, 1), lambda a: (0, 0)),
            pl.BlockSpec((beliefs, width), lambda a: (0, 0)),
            pl.BlockSpec((1, 1, width), lambda a: (a, 0, 0)),
            pl.BlockSpec((1, width, states), lambda a: (a, 0, 0)),
        ],
        out_specs=pl.BlockSpec((beliefs, states), lambda a: (0, 0)),
        compiler_params=pltpu.CompilerParams(
            vmem_limit_bytes=48 << 20, dimension_semantics=("arbitrary",)
        ),
        cost_estimate=pl.CostEstimate(
            flops=4 * beliefs * width * actions * states,
            bytes_accessed=2 * actions * width * states,
            transcendentals=0,
        ),
        name="move",
    )(acts[:, None], weighted, totals[:, None, :], table)


def action_table(actions, count):
    return (actions[:, None] == jnp.arange(count, dtype=jnp.int32)[None, :]).astype(jnp.float32)


MESH = pl.DeviceIdType.MESH
code_top = 32767.0


def encode(values, top):
    q = (values * (code_top / top) + (code_top + 1.5)).astype(jnp.int32) - 32768
    return q.astype(jnp.int16)


def column_top(blocks):
    tops = [jnp.max(jnp.abs(v), axis=0, keepdims=True) for v in blocks]
    return jnp.maximum(functools.reduce(jnp.maximum, tops), 1e-30)


def decode(codes, scale):
    return codes.astype(jnp.int32).astype(jnp.float32) * scale


def fused_kernel(
    plan,
    picks_ref,
    act_ref,
    actv_ref,
    rew_ref,
    alpha_ref,
    w_ref,
    trans_ref,
    out_ref,
    araw,
    aslab,
    wraw,
    wslab,
    tvm,
    pick_in,
    pick_sm,
    stage,
    totst,
    totrv,
    psend,
    precv,
    pscale_s,
    pscale_r,
    xbig,
    outp,
    ysum,
    xsend,
    xrecv,
    xscale_s,
    xscale_r,
    zsend,
    zrecv,
    zscale_s,
    zscale_r,
    tpart,
    tz,
    tx,
    rsel,
    tsel,
    loc_sem,
    tr_sem,
    a_ys,
    a_yr,
    a_ps,
    a_pr,
    a_fs,
    a_fr,
    w_xs,
    w_xr,
    w_fs,
    w_fr,
    pk_s,
    pk_r,
    pk_l,
    tt_zs,
    tt_zr,
    tt_xs,
    tt_xr,
    tot_s,
    tot_r,
    p_s,
    p_r,
    ps_s,
    ps_r,
    x_s,
    x_r,
    xs_s,
    xs_r,
    z_s,
    z_r,
    zs_s,
    zs_r,
):
    ranks, groups, actions, obs_local, rows, cols, beliefs, chunk, width = plan
    zs, ys = ranks // 2, groups // 2
    sps = cols // lanes
    slabs = zs * sps
    owned = beliefs // ranks
    half_obs = obs_local // 2
    per_row = lanes // obs_local
    chunks = beliefs // chunk
    steps = zs * 2 * cols // width

    me_o, me_b = lax.axis_index("obs"), lax.axis_index("bel")
    z, x = lax.div(me_o, 2), lax.rem(me_o, 2)
    y, c = lax.div(me_b, 2), lax.rem(me_b, 2)
    x_peer = {"obs": me_o + 1 - 2 * x}
    core_peer = {"bel": me_b + 1 - 2 * c}
    z_at = [lax.rem(z + d, zs) for d in range(zs)]
    z_peer = [{"obs": zt * 2 + x} for zt in z_at]
    y_peer = [{"bel": lax.rem(y + d, ys) * 2 + c} for d in range(ys)]
    y_from = [lax.rem(y + ys - d, ys) for d in range(ys)]

    def remote(src, dst, s_sem, r_sem, where):
        return pltpu.make_async_remote_copy(
            src_ref=src,
            dst_ref=dst,
            send_sem=s_sem,
            recv_sem=r_sem,
            device_id=where,
            device_id_type=MESH,
        )

    def band(s):
        return pl.ds(s * cols, cols)

    def source_band(s, side):
        return pl.ds(pl.multiple_of((2 * s + side) * cols, cols), cols)

    own_w = [
        pltpu.make_async_copy(
            w_ref.at[:, :, source_band(s, x)], wraw.at[0, :, :, band(s)], loc_sem.at[0, s]
        )
        for s in range(zs)
    ]
    own_a = [
        pltpu.make_async_copy(
            alpha_ref.at[:, source_band(s, x)], araw.at[me_b, :, band(s)], loc_sem.at[1, s]
        )
        for s in range(zs)
    ]
    table = [
        pltpu.make_async_copy(
            trans_ref.at[:, pl.ds(n * width, width)], tvm.at[n], tr_sem.at[n]
        )
        for n in range(steps)
    ]
    own_pick = pltpu.make_async_copy(picks_ref, pick_sm.at[0], pk_l.at[0])
    for copy in own_w:
        copy.start()
    own_pick.start()
    for copy in own_a:
        copy.start()
    for copy in table:
        copy.start()

    peers = [x_peer, core_peer] + z_peer[1:] + y_peer[1:]
    barrier = pltpu.get_barrier_semaphore()
    for peer in peers:
        pl.semaphore_signal(barrier, inc=1, device_id=peer, device_id_type=MESH)
    pl.semaphore_wait(barrier, len(peers))

    def half(side):
        return pl.ds(side * half_obs, half_obs)

    pick_copy = remote(picks_ref, pick_in, pk_s, pk_r, x_peer)
    pick_copy.start()
    w_out, a_out, a_core = [], [], []
    for s in range(zs):
        w_out.append(
            remote(
                w_ref.at[half(c), :, source_band(s, 1 - x)],
                wraw.at[1, half(c), :, band(s)],
                w_xs.at[s],
                w_xr.at[s],
                x_peer,
            )
        )
        w_out[-1].start()
        for d in range(1, ys):
            a_out.append(
                remote(
                    alpha_ref.at[:, source_band(s, x)],
                    araw.at[me_b, :, band(s)],
                    a_ys.at[d - 1, s],
                    a_yr.at[d - 1, s],
                    y_peer[d],
                )
            )
            a_out[-1].start()
    for s in range(zs):
        a_core.append(
            remote(
                alpha_ref.at[:, source_band(s, x)],
                araw.at[me_b, :, band(s)],
                a_ps.at[s],
                a_pr.at[s],
                core_peer,
            )
        )
        a_core[-1].start()

    for n in range(steps):
        table[n].wait()

        def column_total(a, carry, n=n):
            part = tvm[n, pl.ds(pl.multiple_of(a * cols, cols), cols), :].astype(jnp.float32)
            tpart[pl.ds(a, 1), n * width : (n + 1) * width] = jnp.sum(
                part, axis=0, keepdims=True
            )
            return carry

        lax.fori_loop(0, actions, column_total, 0)
    tt_out = [
        remote(tpart, tz.at[d - 1], tt_zs.at[d - 1], tt_zr.at[d - 1], z_peer[d])
        for d in range(1, zs)
    ]
    for copy in tt_out:
        copy.start()

    def weight_slab(p, obs_from, s):
        def one(o, carry):
            o = o + obs_from
            for a in range(0, actions, 8):
                for h in range(sps):
                    at = s * cols + h * lanes
                    value = wraw[p, o, a : a + 8, at : at + lanes]
                    first = ((p * obs_local + o) * actions + a) * slabs + s * sps + h
                    wslab[pl.ds(first, 8, stride=slabs), :] = value
            return carry

        lax.fori_loop(0, half_obs, one, 0)

    def alpha_slab(member, s):
        def one(r, carry):
            for k in range(2):
                r0 = pl.multiple_of(r * 32 + k * 16, 16)
                for h in range(sps):
                    at = s * cols + h * lanes
                    value = araw[member, pl.ds(r0, 16), at : at + lanes].astype(jnp.float32)
                    first = (member * rows + r0) * slabs + s * sps + h
                    aslab[pl.ds(first, 16, stride=slabs), :] = value
            return carry

        lax.fori_loop(0, rows // 32, one, 0)

    for s in range(zs):
        own_w[s].wait()
        weight_slab(0, 0, s)
        weight_slab(0, half_obs, s)
    for s in range(zs):
        own_a[s].wait()
        alpha_slab(me_b, s)

    for copy in tt_out:
        copy.wait()
    total = tpart[...]
    for d in range(1, zs):
        total = total + tz[d - 1]
    tx[0] = total
    tx_out = remote(tx.at[0], tx.at[1], tt_xs, tt_xr, x_peer)
    tx_out.start()

    other = me_b + 1 - 2 * c
    for s in range(zs):
        a_core[s].wait_recv()
        alpha_slab(other, s)

    forwards = []
    for s in range(zs):
        w_out[s].wait_recv()
        forwards.append(
            remote(
                wraw.at[1, half(c), :, band(s)],
                wraw.at[1, half(c), :, band(s)],
                w_fs.at[s],
                w_fr.at[s],
                core_peer,
            )
        )
        forwards[-1].start()
        a_forward = []
        for d in range(1, ys):
            member = y_from[d] * 2 + c
            slot = araw.at[member, :, band(s)]
            remote(slot, slot, a_ys.at[d - 1, s], a_yr.at[d - 1, s], y_peer[d]).wait_recv()
            a_forward.append(remote(slot, slot, a_fs.at[d - 1, s], a_fr.at[d - 1, s], core_peer))
            a_forward[-1].start()
        weight_slab(1, c * half_obs, s)
        for d in range(1, ys):
            alpha_slab(y_from[d] * 2 + c, s)
        forwards[-1].wait_recv()
        weight_slab(1, (1 - c) * half_obs, s)
        for d in range(1, ys):
            a_forward[d - 1].wait_recv()
            alpha_slab(y_from[d] * 2 + 1 - c, s)
        forwards += a_forward

    own_pick.wait()
    pick_copy.wait()
    peer_pick = pltpu.make_async_copy(pick_in, pick_sm.at[1], pk_l.at[1])
    peer_pick.start()
    tx_out.wait()

    def obs_total(a, carry):
        sums = [None] * 4
        for o in range(2 * obs_local):
            term = wslab[pl.ds(pl.multiple_of((o * actions + a) * slabs, slabs), slabs), :]
            sums[o % 4] = term if sums[o % 4] is None else sums[o % 4] + term
        totst[pl.ds(a, slabs, stride=actions), :] = (sums[0] + sums[1]) + (sums[2] + sums[3])
        return carry

    lax.fori_loop(0, actions, obs_total, 0)
    tot_rows = sps * actions
    tot_out = [
        remote(
            totst.at[pl.ds(pl.multiple_of(z_at[d] * tot_rows, 8), tot_rows)],
            totrv.at[d - 1],
            tot_s.at[d - 1],
            tot_r.at[d - 1],
            z_peer[d],
        )
        for d in range(1, zs)
    ]
    for copy in tot_out:
        copy.start()
    peer_pick.wait()

    p_out = []
    for q in range(chunks):

        def one(r, carry):
            for t in range(per_row):
                b = r * per_row + t
                base = act_ref[b] * slabs
                sums = [None] * 4
                for p in range(2):
                    for o in range(obs_local):
                        row = aslab[
                            pl.ds(pick_sm[p, r, t * obs_local + o], slabs), :
                        ]
                        at = (p * obs_local + o) * actions * slabs
                        weight = wslab[pl.ds(base + at, slabs), :]
                        term = row * weight
                        k = o % 4
                        sums[k] = term if sums[k] is None else sums[k] + term
                stage[pl.ds(b, slabs, stride=beliefs), :] = (sums[0] + sums[1]) + (
                    sums[2] + sums[3]
                )
            return carry

        per_chunk = chunk // per_row
        lax.fori_loop(q * per_chunk, (q + 1) * per_chunk, one, 0)
        for d in range(1, zs):
            for h in range(sps):
                first = (z_at[d] * sps + h) * beliefs + q * chunk
                value = stage[pl.ds(pl.multiple_of(first, 8), chunk), :]
                top = column_top([value])
                psend[q, d - 1, h] = encode(value, top)
                pscale_s[q, d - 1, h : h + 1, :] = top * (1.0 / code_top)
            here = (q, d - 1)
            p_out.append(remote(psend.at[here], precv.at[here], p_s.at[here], p_r.at[here], z_peer[d]))
            p_out.append(
                remote(
                    pscale_s.at[here], pscale_r.at[here], ps_s.at[here], ps_r.at[here], z_peer[d]
                )
            )
            p_out[-1].start()
            p_out[-2].start()

    own_act = actv_ref[pl.ds(pl.multiple_of(me_o * owned, 8), owned), :]
    block = min(512, rsel.shape[1])
    for at in range(0, rsel.shape[1], block):
        reward = jnp.zeros((owned, block), jnp.float32)
        scale = jnp.zeros((owned, block), jnp.float32)
        for a in range(actions):
            hit = own_act == a
            both = tx[0, a : a + 1, at : at + block] + tx[1, a : a + 1, at : at + block]
            reward = jnp.where(hit, rew_ref[a : a + 1, at : at + block], reward)
            scale = jnp.where(hit, both, scale)
        rsel[:, at : at + block] = reward
        tsel[:, at : at + block] = discount / scale

    for copy in tot_out:
        copy.wait()
    totals = totst[pl.ds(pl.multiple_of(z * tot_rows, 8), tot_rows), :]
    for d in range(1, zs):
        totals = totals + totrv[d - 1]

    for q in range(chunks):
        for copy in p_out[2 * (zs - 1) * q : 2 * (zs - 1) * (q + 1)]:
            copy.wait()
        b0 = q * chunk
        act = jnp.broadcast_to(actv_ref[b0 : b0 + chunk, :], (chunk, lanes))
        for h in range(sps):
            first = (z * sps + h) * beliefs + b0
            value = stage[pl.ds(pl.multiple_of(first, 8), chunk), :]
            for d in range(1, zs):
                value = value + decode(precv[q, d - 1, h], pscale_r[q, d - 1, h : h + 1, :])
            under = jnp.ones_like(value)
            for a in range(actions):
                at = h * actions + a
                under = jnp.where(act == a, totals[at : at + 1, :], under)
            value = value / under
            high = value.astype(jnp.bfloat16).astype(jnp.float32)
            low = value - high
            for a in range(actions):
                at = a * cols + h * lanes
                hit = act == a
                xbig[b0 : b0 + chunk, at : at + lanes] = jnp.where(hit, high, 0.0).astype(
                    jnp.bfloat16
                )
                xbig[beliefs + b0 : beliefs + b0 + chunk, at : at + lanes] = jnp.where(
                    hit, low, 0.0
                ).astype(jnp.bfloat16)

    def x_copies(n):
        return (
            remote(xsend.at[n], xrecv.at[n], x_s.at[n], x_r.at[n], x_peer),
            remote(xscale_s.at[n], xscale_r.at[n], xs_s.at[n], xs_r.at[n], x_peer),
        )

    def z_copies(n, d):
        here = (n, d - 1)
        return (
            remote(zsend.at[here], zrecv.at[here], z_s.at[here], z_r.at[here], z_peer[d]),
            remote(zscale_s.at[here], zscale_r.at[here], zs_s.at[here], zs_r.at[here], z_peer[d]),
        )

    def owner_rows(zt, side):
        return pl.ds(pl.multiple_of((2 * zt + side) * owned, 8), owned)

    def to_pair(n):
        sides = [outp[n, owner_rows(s, 1 - x), :] for s in range(zs)]
        top = column_top(sides)
        for s in range(zs):
            xsend[n, s * owned : (s + 1) * owned, :] = encode(sides[s], top)
        xscale_s[n] = top * (1.0 / code_top)
        for copy in x_copies(n):
            copy.start()

    def to_owners(n):
        for copy in x_copies(n):
            copy.wait()
        scale = xscale_r[n]
        for s in range(zs):
            part = slice(s * owned, (s + 1) * owned)
            ysum[n, part, :] = outp[n, owner_rows(s, x), :] + decode(xrecv[n, part, :], scale)
        for d in range(1, zs):
            value = ysum[n, pl.ds(pl.multiple_of(z_at[d] * owned, 8), owned), :]
            top = column_top([value])
            zsend[n, d - 1] = encode(value, top)
            zscale_s[n, d - 1] = top * (1.0 / code_top)
            for copy in z_copies(n, d):
                copy.start()

    def finish(n):
        value = ysum[n, pl.ds(pl.multiple_of(z * owned, 8), owned), :]
        for d in range(1, zs):
            for copy in z_copies(n, d):
                copy.wait()
            value = value + decode(zrecv[n, d - 1], zscale_r[n, d - 1])
        at = pl.ds(pl.multiple_of(n * width, width), width)
        out_ref[:, at] = rsel[:, at] + value * tsel[:, at]

    lag = min(3, steps)

    def step(n, carry):
        both = jnp.dot(xbig[...], tvm[n], preferred_element_type=jnp.float32)
        outp[n] = both[:beliefs] + both[beliefs:]
        to_pair(n)

        @pl.when(n >= 1)
        def _():
            to_owners(n - 1)

        @pl.when(n >= lag)
        def _():
            finish(n - lag)

        return carry

    lax.fori_loop(0, steps, step, 0)
    to_owners(steps - 1)
    for n in range(steps - lag, steps):
        finish(n)
    for copy in w_out + a_out + a_core + forwards:
        copy.wait_send()


def fused(alpha_set, transitions, obs_weights, rewards, picks, chosen_action, groups):
    actions, states = rewards.shape
    obs_local = obs_weights.shape[0]
    beliefs = chosen_action.shape[0]
    ranks = lax.axis_size("obs")
    rows = alpha_set.shape[0]
    cols = states // ranks
    zs, ys = ranks // 2, groups // 2
    sps = cols // lanes
    slabs = zs * sps
    owned = beliefs // ranks
    chunk = beliefs // 4
    chunks = beliefs // chunk
    width = 256
    steps = states // width
    xc = zs * cols
    plan = (ranks, groups, actions, obs_local, rows, cols, beliefs, chunk, width)
    f32, bf16, i16, i32 = jnp.float32, jnp.bfloat16, jnp.int16, jnp.int32
    vmem, dma = pltpu.VMEM, pltpu.SemaphoreType.DMA
    pick_rows = beliefs * obs_local // lanes
    scratch = [
        vmem((groups, rows, xc), bf16),
        vmem((groups * rows * slabs, lanes), f32),
        vmem((2, obs_local, actions, xc), f32),
        vmem((2 * obs_local * actions * slabs, lanes), f32),
        vmem((steps, actions * cols, width), bf16),
        vmem((pick_rows, lanes), i32),
        pltpu.SMEM((2, pick_rows, lanes), i32),
        vmem((slabs * beliefs, lanes), f32),
        vmem((slabs * actions, lanes), f32),
        vmem((zs - 1, sps * actions, lanes), f32),
        vmem((chunks, zs - 1, sps, chunk, lanes), i16),
        vmem((chunks, zs - 1, sps, chunk, lanes), i16),
        vmem((chunks, zs - 1, sps, lanes), f32),
        vmem((chunks, zs - 1, sps, lanes), f32),
        vmem((2 * beliefs, actions * cols), bf16),
        vmem((steps, beliefs, width), f32),
        vmem((steps, zs * owned, width), f32),
        vmem((steps, zs * owned, width), i16),
        vmem((steps, zs * owned, width), i16),
        vmem((steps, 1, width), f32),
        vmem((steps, 1, width), f32),
        vmem((steps, zs - 1, owned, width), i16),
        vmem((steps, zs - 1, owned, width), i16),
        vmem((steps, zs - 1, 1, width), f32),
        vmem((steps, zs - 1, 1, width), f32),
        vmem((actions, states), f32),
        vmem((zs - 1, actions, states), f32),
        vmem((2, actions, states), f32),
        vmem((owned, states), f32),
        vmem((owned, states), f32),
        dma((2, zs)),
        dma((steps,)),
        dma((max(ys - 1, 1), zs)),
        dma((max(ys - 1, 1), zs)),
        dma((zs,)),
        dma((zs,)),
        dma((max(ys - 1, 1), zs)),
        dma((max(ys - 1, 1), zs)),
        dma((zs,)),
        dma((zs,)),
        dma((zs,)),
        dma((zs,)),
        dma(()),
        dma(()),
        dma((2,)),
        dma((zs - 1,)),
        dma((zs - 1,)),
        dma(()),
        dma(()),
        dma((zs - 1,)),
        dma((zs - 1,)),
        dma((chunks, zs - 1)),
        dma((chunks, zs - 1)),
        dma((chunks, zs - 1)),
        dma((chunks, zs - 1)),
        dma((steps,)),
        dma((steps,)),
        dma((steps,)),
        dma((steps,)),
        dma((steps, zs - 1)),
        dma((steps, zs - 1)),
        dma((steps, zs - 1)),
        dma((steps, zs - 1)),
    ]
    hbm = pl.BlockSpec(memory_space=pl.ANY)
    local = pl.BlockSpec(memory_space=pltpu.VMEM)
    return pl.pallas_call(
        functools.partial(fused_kernel, plan),
        out_shape=jax.ShapeDtypeStruct((owned, states), f32),
        in_specs=[hbm, pl.BlockSpec(memory_space=pltpu.SMEM), local, local, hbm, hbm, hbm],
        out_specs=local,
        scratch_shapes=scratch,
        compiler_params=pltpu.CompilerParams(
            collective_id=0, has_side_effects=True, vmem_limit_bytes=67043328
        ),
        name="backup",
    )(
        (picks * slabs).reshape(pick_rows, lanes),
        chosen_action,
        chosen_action[:, None],
        rewards,
        alpha_set,
        obs_weights,
        transitions.reshape(actions * cols, states),
    )


def fits(alpha_set, transitions, obs_weights, beliefs, ranks, groups):
    cols = transitions.shape[1]
    obs_local, actions, states = obs_weights.shape
    return (
        ranks % 2 == 0
        and ranks > 2
        and groups % 2 == 0
        and cols % lanes == 0
        and states == ranks * cols
        and states % 256 == 0
        and actions % 8 == 0
        and obs_local % 2 == 0
        and lanes % obs_local == 0
        and alpha_set.shape[0] % 32 == 0
        and beliefs % (16 * ranks) == 0
        and beliefs % 64 == 0
    )


def body(alpha_set, transitions, obs_weights, rewards, chosen_idx, chosen_action):
    actions, states = rewards.shape
    obs_local = obs_weights.shape[0]
    beliefs = chosen_action.shape[0]
    slabs = states // lanes
    ranks = lax.axis_size("obs")
    action_hot = action_table(chosen_action, actions)
    picks = jnp.sum(jnp.where(action_hot[:, :, None] > 0, chosen_idx, 0), axis=1).reshape(-1)
    groups = lax.axis_size("bel")
    if fits(alpha_set, transitions, obs_weights, beliefs, ranks, groups):
        return fused(
            alpha_set, transitions, obs_weights, rewards, picks, chosen_action, groups
        )
    alpha = lax.all_gather(alpha_set.reshape(-1, slabs, lanes), "bel", axis=0, tiled=True)
    weights = obs_weights.reshape(obs_local * actions, slabs, lanes)
    trans_part = jnp.sum(transitions.astype(jnp.float32), axis=1).reshape(actions, slabs, lanes)
    partial = gather_rows(picks, chosen_action, alpha, weights, trans_part)
    rows = partial.shape[1]
    if slabs % ranks == 0:
        piece = lax.psum_scatter(partial, "obs", scatter_dimension=0, tiled=True)
        piece = piece.transpose(1, 0, 2).reshape(rows, -1)
    else:
        flat = partial.transpose(1, 0, 2).reshape(rows, states)
        piece = lax.psum_scatter(flat, "obs", scatter_dimension=1, tiled=True)
    trans_totals = lax.all_gather(piece[beliefs + actions :], "obs", axis=1, tiled=True)
    moved = move(
        chosen_action, piece[:beliefs], piece[beliefs : beliefs + actions], transitions
    )
    future = lax.psum_scatter(moved, "obs", scatter_dimension=0, tiled=True)
    owned = beliefs // ranks
    own_hot = lax.dynamic_slice_in_dim(action_hot, lax.axis_index("obs") * owned, owned, 0)
    own = functools.partial(
        jnp.dot, own_hot, precision=lax.Precision.HIGHEST, preferred_element_type=jnp.float32
    )
    return own(rewards) + discount * (future / own(trans_totals))


def solution(mesh):
    placed = (
        P("bel", None),
        P(None, "obs", None),
        P("obs", None, None),
        P(),
        P("bel", None, "obs"),
        P("bel"),
    )
    return jax.shard_map(
        body, mesh=mesh, in_specs=placed, out_specs=P(("bel", "obs"), None), check_vma=False
    )
```

```python
import functools
import types

import jax
import jax.numpy as jnp
from jax import lax
from jax.experimental import pallas as pl
from jax.experimental.pallas import tpu as pltpu
from jax.sharding import PartitionSpec as P

discount = 0.95
lanes = 128


def gather_kernel(picks_ref, act_ref, alpha_ref, weights_ref, moves_ref, out_ref):
    beliefs = act_ref.shape[0]
    obs_local = picks_ref.shape[0] // beliefs
    actions = weights_ref.shape[0] // obs_local
    slabs = alpha_ref.shape[1]
    rows = out_ref.shape[0] // slabs

    def one(b, carry):
        action = act_ref[b]
        sums = [None] * min(4, obs_local)
        for o in range(obs_local):
            row = alpha_ref[picks_ref[b * obs_local + o]].astype(jnp.float32)
            term = row * weights_ref[o * actions + action]
            at = o % len(sums)
            sums[at] = term if sums[at] is None else sums[at] + term
        out_ref[pl.ds(b, slabs, stride=rows), :] = functools.reduce(jnp.add, sums)
        return carry

    lax.fori_loop(0, beliefs, one, 0)

    def total(a, carry):
        acc = weights_ref[a]
        for o in range(1, obs_local):
            acc = acc + weights_ref[o * actions + a]
        out_ref[pl.ds(beliefs + a, slabs, stride=rows), :] = acc
        out_ref[pl.ds(beliefs + actions + a, slabs, stride=rows), :] = moves_ref[a]
        return carry

    lax.fori_loop(0, actions, total, 0)


def gather_rows(picks, acts, alpha, weights, moves):
    slabs = alpha.shape[1]
    beliefs = acts.shape[0]
    rows = beliefs + 2 * moves.shape[0]
    vmem = pl.BlockSpec(memory_space=pltpu.VMEM)
    smem = pl.BlockSpec(memory_space=pltpu.SMEM)
    out = pl.pallas_call(
        gather_kernel,
        out_shape=jax.ShapeDtypeStruct((slabs * rows, lanes), jnp.float32),
        in_specs=[smem, smem, vmem, vmem, vmem],
        out_specs=vmem,
        compiler_params=pltpu.CompilerParams(vmem_limit_bytes=40 << 20),
        cost_estimate=pl.CostEstimate(
            flops=80_000_000, bytes_accessed=16 << 20, transcendentals=0
        ),
        name="gather_rows",
    )(picks, acts, alpha, weights, moves)
    return out.reshape(slabs, rows, lanes)


def move_kernel(act_ref, w_ref, tot_ref, table_ref, out_ref):
    a = pl.program_id(0)
    scaled = w_ref[...] / tot_ref[0]
    x = jnp.where(act_ref[...] == a, scaled, 0.0)
    high = x.astype(jnp.bfloat16)
    low = (x - high.astype(jnp.float32)).astype(jnp.bfloat16)
    table = table_ref[0]
    both = jnp.dot(jnp.concatenate([high, low], axis=0), table, preferred_element_type=jnp.float32)
    half = x.shape[0]
    part = both[:half] + both[half:]

    @pl.when(a == 0)
    def _():
        out_ref[...] = part

    @pl.when(a > 0)
    def _():
        out_ref[...] += part


def move(acts, weighted, totals, table):
    beliefs, width = weighted.shape
    actions, _, states = table.shape
    return pl.pallas_call(
        move_kernel,
        grid=(actions,),
        out_shape=jax.ShapeDtypeStruct((beliefs, states), jnp.float32),
        in_specs=[
            pl.BlockSpec((beliefs, 1), lambda a: (0, 0)),
            pl.BlockSpec((beliefs, width), lambda a: (0, 0)),
            pl.BlockSpec((1, 1, width), lambda a: (a, 0, 0)),
            pl.BlockSpec((1, width, states), lambda a: (a, 0, 0)),
        ],
        out_specs=pl.BlockSpec((beliefs, states), lambda a: (0, 0)),
        compiler_params=pltpu.CompilerParams(
            vmem_limit_bytes=48 << 20, dimension_semantics=("arbitrary",)
        ),
        cost_estimate=pl.CostEstimate(
            flops=4 * beliefs * width * actions * states,
            bytes_accessed=2 * actions * width * states,
            transcendentals=0,
        ),
        name="move",
    )(acts[:, None], weighted, totals[:, None, :], table)


def action_table(actions, count):
    return (actions[:, None] == jnp.arange(count, dtype=jnp.int32)[None, :]).astype(jnp.float32)


MESH = pl.DeviceIdType.MESH
code_top = 32767.0


def encode(values, top):
    q = (values * (code_top / top) + (code_top + 1.5)).astype(jnp.int32) - 32768
    return q.astype(jnp.int16)


def column_top(blocks):
    tops = [jnp.max(jnp.abs(v), axis=0, keepdims=True) for v in blocks]
    return jnp.maximum(functools.reduce(jnp.maximum, tops), 1e-30)


def decode(codes, scale):
    return codes.astype(jnp.int32).astype(jnp.float32) * scale


def fused_kernel(plan, names, *refs):
    r = types.SimpleNamespace(**dict(zip(names, refs)))
    ranks, groups, actions, obs_local, rows, cols, beliefs, chunk, width = plan
    zs, ys = ranks // 2, groups // 2
    sps = cols // lanes
    slabs = zs * sps
    owned = beliefs // ranks
    half_obs = obs_local // 2
    chunks = beliefs // chunk
    steps = zs * 2 * cols // width
    share = steps // groups
    parts = r.a_yr.shape[2]
    part_rows = rows // parts
    pairs = zs // 2

    me_o, me_b = lax.axis_index("obs"), lax.axis_index("bel")
    z, x = lax.div(me_o, 2), lax.rem(me_o, 2)
    y, c = lax.div(me_b, 2), lax.rem(me_b, 2)
    odd = lax.rem(z, 2)
    other = me_b + 1 - 2 * c
    x_peer = {"obs": me_o + 1 - 2 * x}
    core_peer = {"bel": other}
    next_z = {"obs": (z + 1 - 2 * odd) * 2 + x}
    z_at = [lax.rem(z + d, zs) for d in range(zs)]
    z_peer = [{"obs": zt * 2 + x} for zt in z_at]
    y_peer = [{"bel": lax.rem(y + d, ys) * 2 + c} for d in range(ys)]
    y_from = [lax.rem(y + ys - d, ys) for d in range(ys)]
    b_peer = [{"bel": lax.rem(me_b + d, groups)} for d in range(groups)]
    b_from = [lax.rem(me_b + groups - d, groups) for d in range(groups)]

    def remote(src, dst, s_sem, r_sem, where):
        return pltpu.make_async_remote_copy(
            src_ref=src,
            dst_ref=dst,
            send_sem=s_sem,
            recv_sem=r_sem,
            device_id=where,
            device_id_type=MESH,
        )

    def band(s):
        return pl.ds(pl.multiple_of(s * cols, lanes), cols)

    def source_band(s, side):
        return pl.ds(pl.multiple_of((2 * s + side) * cols, lanes), cols)

    def half(side):
        return pl.ds(side * half_obs, half_obs)

    own_idx = pltpu.make_async_copy(r.idx, r.idx_in, r.pk_l.at[2 * obs_local])
    peer_w = [
        pltpu.make_async_copy(
            r.weights.at[half(c), :, source_band(s, 1 - x)], r.w_src.at[s], r.loc_sem.at[2, s]
        )
        for s in range(zs)
    ]
    own_w = [
        pltpu.make_async_copy(
            r.weights.at[:, :, source_band(s, x)], r.wraw.at[:, :, band(s)], r.loc_sem.at[0, s]
        )
        for s in range(zs)
    ]
    own_a = [
        pltpu.make_async_copy(
            r.alpha.at[:, source_band(s, x)], r.araw.at[me_b, :, band(s)], r.loc_sem.at[1, s]
        )
        for s in range(zs)
    ]
    table = []
    for k in range(steps):
        n = lax.rem(me_b * share + k, steps)
        at = pl.ds(pl.multiple_of(n * width, lanes), width)
        table.append(pltpu.make_async_copy(r.trans.at[:, at], r.tvm.at[n], r.tr_sem.at[k]))
    for copy in peer_w + [own_idx] + own_w + table[:share] + own_a + table[share:]:
        copy.start()

    peers = [x_peer] + z_peer[1:] + b_peer[1:]
    barrier = pltpu.get_barrier_semaphore()
    for peer in peers:
        pl.semaphore_signal(barrier, inc=1, device_id=peer, device_id_type=MESH)
    pl.semaphore_wait(barrier, len(peers))

    def rows_of(h):
        return pl.ds(h * part_rows, part_rows)

    def near(k):
        return 2 * k + odd

    def far(k):
        return 2 * k + 1 - odd

    pieces = [(k, h) for k in range(pairs) for h in range(parts)]
    sent = []

    def launch(copy):
        copy.start()
        sent.append(copy)

    for k, h in pieces:
        for d in range(1, ys):
            launch(
                remote(
                    r.alpha.at[rows_of(h), source_band(near(k), x)],
                    r.araw.at[me_b, rows_of(h), band(near(k))],
                    r.a_ys.at[d - 1, k, h],
                    r.a_yr.at[d - 1, k, h],
                    y_peer[d],
                )
            )
    a_core = [
        remote(
            r.alpha.at[:, source_band(s, x)],
            r.araw.at[me_b, :, band(s)],
            r.a_ps.at[s],
            r.a_pr.at[s],
            core_peer,
        )
        for s in range(zs)
    ]
    for copy in a_core:
        launch(copy)

    w_out = []
    for s in range(zs):
        peer_w[s].wait()
        for at in range(0, cols, lanes):
            value = r.w_src[s, :, :, at : at + lanes]
            top = jnp.maximum(jnp.max(jnp.abs(value), axis=0), 1e-30)
            r.w_code_s[s, :, :, at : at + lanes] = encode(value, top[None])
            r.w_scale_s[s, :, at : at + lanes] = top * (1.0 / code_top)
        w_out.append(
            (
                remote(r.w_code_s.at[s], r.w_code.at[c, s], r.w_xs.at[0, s], r.w_xr.at[0, s], x_peer),
                remote(
                    r.w_scale_s.at[s], r.w_scale.at[c, s], r.w_xs.at[1, s], r.w_xr.at[1, s], x_peer
                ),
            )
        )
        for copy in w_out[-1]:
            launch(copy)

    pick_sm = [getattr(r, f"pick_{k}") for k in range(2 * obs_local)]
    waiting = []

    def store_picks(source, first):
        for o in range(obs_local):
            copy = pltpu.make_async_copy(
                source.at[pl.ds(o, 1), :], pick_sm[first + o], r.pk_l.at[first + o]
            )
            copy.start()
            waiting.append(copy)

    def own_picks():
        own_idx.wait()
        action_row = r.act_row[...]
        chosen = jnp.zeros((obs_local, beliefs), jnp.int32)
        for a in range(actions):
            chosen = jnp.where(action_row == a, r.idx_in[a], chosen)
        r.pick_out[...] = chosen * slabs

    pick_copy = remote(r.pick_out, r.pick_in, r.pk_s, r.pk_r, x_peer)
    tt_out = [
        remote(r.tpart, r.tz.at[d - 1], r.tt_zs.at[d - 1], r.tt_zr.at[d - 1], z_peer[d])
        for d in range(1, zs)
    ]
    tx_out = remote(r.tx.at[0], r.tx.at[1], r.tt_xs, r.tt_xr, x_peer)

    def transition_totals():
        for k in range(share):
            table[k].wait()
            n = me_b * share + k

            def column_total(a, carry, n=n, k=k):
                value = r.tvm[n, pl.ds(pl.multiple_of(a * cols, 16), cols), :].astype(jnp.float32)
                r.tpart[pl.ds(a, 1), k * width : (k + 1) * width] = jnp.sum(
                    value, axis=0, keepdims=True
                )
                return carry

            lax.fori_loop(0, actions, column_total, 0)

    def action_lanes(b, carry):
        r.actb[pl.ds(b, 1), :] = jnp.full((1, lanes), r.act[b], jnp.int32)
        return carry

    pad = slabs

    def own_weight_slab(s):
        def one(o, carry):
            for h in range(sps):
                at = s * cols + h * lanes
                first = o * actions * slabs + s * sps + h + pad
                r.wslab[pl.ds(first, actions, stride=slabs), :] = r.wraw[o, :, at : at + lanes]
            return carry

        lax.fori_loop(0, obs_local, one, 0)

    def peer_weight_slab(side, s):
        def one(o, carry):
            for h in range(sps):
                at = slice(h * lanes, (h + 1) * lanes)
                first = (obs_local + side * half_obs + o) * actions * slabs + s * sps + h + pad
                r.wslab[pl.ds(first, actions, stride=slabs), :] = decode(
                    r.w_code[side, s, o, :, at], r.w_scale[side, s, :, at]
                )
            return carry

        lax.fori_loop(0, half_obs, one, 0)

    def alpha_slab(member, s, first_row, count):
        def one(i, carry):
            for k in range(2):
                r0 = pl.multiple_of(first_row + i * 32 + k * 16, 16)
                for h in range(sps):
                    at = pl.ds(pl.multiple_of(s * cols + h * lanes, lanes), lanes)
                    first = (member * rows + r0) * slabs + s * sps + h
                    r.aslab[pl.ds(first, 16, stride=slabs), :] = r.araw[
                        member, pl.ds(r0, 16), at
                    ].astype(jnp.float32)
            return carry

        lax.fori_loop(0, count // 32, one, 0)

    late = []

    def arrived(k, h, by_z):
        s = far(k) if by_z else near(k)
        for d in range(1, ys):
            member = y_from[d] * 2 + c
            slot = r.araw.at[member, rows_of(h), band(s)]
            here = (d - 1, k, h)
            if by_z:
                remote(slot, slot, r.a_zs.at[here], r.a_zr.at[here], next_z).wait_recv()
            else:
                remote(slot, slot, r.a_ys.at[here], r.a_yr.at[here], y_peer[d]).wait_recv()
                launch(remote(slot, slot, r.a_zs.at[here], r.a_zr.at[here], next_z))
            at = (d - 1, int(by_z), k, h)
            forward = remote(slot, slot, r.a_fs.at[at], r.a_fr.at[at], core_peer)
            launch(forward)
            alpha_slab(member, s, h * part_rows, part_rows)

            def rest(forward=forward, member=y_from[d] * 2 + 1 - c):
                forward.wait_recv()
                alpha_slab(member, s, h * part_rows, part_rows)

            late.append(rest)

    def weights_arrived(s):
        both = []
        for k, copy in enumerate(w_out[s]):
            copy.wait_recv()
            held = (r.w_code, r.w_scale)[k].at[c, s]
            both.append(remote(held, held, r.w_fs.at[k, s], r.w_fr.at[k, s], core_peer))
            launch(both[-1])
        peer_weight_slab(c, s)

        def rest():
            for copy in both:
                copy.wait_recv()
            peer_weight_slab(1 - c, s)

        late.append(rest)

    count = len(pieces)
    for i in range(count + 1):
        ready, late = late, []
        if i < count:
            arrived(*pieces[i], False)
        if i >= 1:
            arrived(*pieces[i - 1], True)
        for s in range(i * zs // (count + 1), (i + 1) * zs // (count + 1)):
            weights_arrived(s)
        for rest in ready:
            rest()
        if i == 0:
            own_picks()
            for s in range(zs):
                own_w[s].wait()
                own_weight_slab(s)
            pick_copy.start()
            store_picks(r.pick_out, 0)
            for s in range(zs):
                own_a[s].wait()
                alpha_slab(me_b, s, 0, rows)
        if i == 1:
            transition_totals()
            for s in range(zs):
                a_core[s].wait_recv()
                alpha_slab(other, s, 0, rows)
            for copy in tt_out:
                copy.start()
        if i == 2:
            pick_copy.wait()
            store_picks(r.pick_in, obs_local)
            lax.fori_loop(0, beliefs, action_lanes, 0, unroll=8)
    for rest in late:
        rest()
    for copy in tt_out:
        copy.wait()
    total = r.tpart[...]
    for d in range(1, zs):
        total = total + r.tz[d - 1]
    r.tx[0] = total

    def obs_total(a, carry):
        sums = [None] * 4
        for o in range(2 * obs_local):
            term = r.wslab[pl.ds(pl.multiple_of((o * actions + a) * slabs + pad, slabs), slabs), :]
            sums[o % 4] = term if sums[o % 4] is None else sums[o % 4] + term
        r.totst[pl.ds(a, slabs, stride=actions), :] = (sums[0] + sums[1]) + (sums[2] + sums[3])
        return carry

    lax.fori_loop(0, actions, obs_total, 0)
    tot_rows = sps * actions
    tot_out = [
        remote(
            r.totst.at[pl.ds(pl.multiple_of(z_at[d] * tot_rows, 8), tot_rows)],
            r.totrv.at[d - 1],
            r.tot_s.at[d - 1],
            r.tot_r.at[d - 1],
            z_peer[d],
        )
        for d in range(1, zs)
    ]
    tall_out = [
        remote(
            r.tall.at[me_b], r.tall.at[me_b], r.tall_s.at[d - 1], r.tall_r.at[d - 1], b_peer[d]
        )
        for d in range(1, groups)
    ]
    for copy in tot_out + [tx_out]:
        copy.start()
    for copy in waiting:
        copy.wait()

    def share_totals():
        tx_out.wait()
        r.tall[me_b] = r.tx[0] + r.tx[1]
        for copy in tall_out:
            copy.start()

    def p_copies(q, d):
        here = (q, d - 1)
        return (
            remote(r.psend.at[here], r.precv.at[here], r.p_s.at[here], r.p_r.at[here], z_peer[d]),
            remote(
                r.pscale_s.at[here], r.pscale_r.at[here], r.ps_s.at[here], r.ps_r.at[here], z_peer[d]
            ),
        )

    unroll = 4

    def gather_chunk(q):
        def one(i, carry):
            for t in range(unroll):
                b = q * chunk + i * unroll + t
                base = r.act[b] * slabs
                sums = [None] * 4
                for p in range(2):
                    for o in range(obs_local):
                        row = r.aslab[pl.ds(pick_sm[p * obs_local + o][0, b], slabs), :]
                        at = (p * obs_local + o) * actions * slabs + pad
                        term = row * r.wslab[pl.ds(base + at, slabs), :]
                        k = o % 4
                        sums[k] = term if sums[k] is None else sums[k] + term
                r.stage[pl.ds(b, slabs, stride=beliefs), :] = (sums[0] + sums[1]) + (
                    sums[2] + sums[3]
                )
            return carry

        lax.fori_loop(0, chunk // unroll, one, 0)
        for d in range(1, zs):
            for h in range(sps):
                first = (z_at[d] * sps + h) * beliefs + q * chunk
                value = r.stage[pl.ds(pl.multiple_of(first, 8), chunk), :]
                top = column_top([value])
                r.psend[q, d - 1, h] = encode(value, top)
                r.pscale_s[q, d - 1, h : h + 1, :] = top * (1.0 / code_top)
            for copy in p_copies(q, d):
                copy.start()

    def prepare():
        for copy in tot_out + tall_out:
            copy.wait()
        totals = r.totst[pl.ds(pl.multiple_of(z * tot_rows, 8), tot_rows), :]
        for d in range(1, zs):
            totals = totals + r.totrv[d - 1]
        r.tsum[...] = totals
        own_act = r.actb[pl.ds(pl.multiple_of(me_o * owned, 8), owned), :]
        per_member = share * width // lanes

        for member in range(groups):
            for k in range(per_member):
                at = slice(k * lanes, (k + 1) * lanes)
                to = slice((member * per_member + k) * lanes, (member * per_member + k + 1) * lanes)
                reward = jnp.zeros((owned, lanes), jnp.float32)
                scale = jnp.ones((owned, lanes), jnp.float32)
                for a in range(actions):
                    hit = own_act == a
                    reward = jnp.where(hit, r.rew[a : a + 1, to], reward)
                    scale = jnp.where(hit, r.tall[member, a : a + 1, at], scale)
                r.rsel[:, to] = reward
                r.tsel[:, to] = discount / scale

    def absorb(q):
        for d in range(1, zs):
            for copy in p_copies(q, d):
                copy.wait()
        b0 = pl.multiple_of(q * chunk, 16)
        act = r.actb[pl.ds(b0, chunk), :]
        for h in range(sps):
            first = (z * sps + h) * beliefs + q * chunk
            value = r.stage[pl.ds(pl.multiple_of(first, 8), chunk), :]
            for d in range(1, zs):
                value = value + decode(r.precv[q, d - 1, h], r.pscale_r[q, d - 1, h : h + 1, :])
            under = jnp.ones_like(value)
            for a in range(actions):
                at = h * actions + a
                under = jnp.where(act == a, r.tsum[at : at + 1, :], under)
            value = value / under
            high = value.astype(jnp.bfloat16).astype(jnp.float32)
            low = value - high
            for a in range(actions):
                at = slice(a * cols + h * lanes, a * cols + (h + 1) * lanes)
                hit = act == a
                r.xbig[pl.ds(b0, chunk), at] = jnp.where(hit, high, 0.0).astype(jnp.bfloat16)
                r.xbig[pl.ds(pl.multiple_of(beliefs + b0, 16), chunk), at] = jnp.where(
                    hit, low, 0.0
                ).astype(jnp.bfloat16)

    behind = min(3, chunks - 1)

    def gather_step(q, carry):
        gather_chunk(q)

        @pl.when(q == 0)
        def _():
            share_totals()

        @pl.when(q == behind - 1)
        def _():
            prepare()

        @pl.when(q >= behind)
        def _():
            absorb(q - behind)

        return carry

    lax.fori_loop(0, chunks, gather_step, 0)

    def absorb_step(q, carry):
        absorb(q)
        return carry

    lax.fori_loop(chunks - behind, chunks, absorb_step, 0)
    for copy in table[share:]:
        copy.wait()

    def x_copies(n):
        return (
            remote(r.xsend.at[n], r.xrecv.at[n], r.x_s.at[n], r.x_r.at[n], x_peer),
            remote(r.xscale_s.at[n], r.xscale_r.at[n], r.xs_s.at[n], r.xs_r.at[n], x_peer),
        )

    def z_copies(n, d):
        here = (n, d - 1)
        return (
            remote(r.zsend.at[here], r.zrecv.at[here], r.z_s.at[here], r.z_r.at[here], z_peer[d]),
            remote(r.zscale_s.at[here], r.zscale_r.at[here], r.zs_s.at[here], r.zs_r.at[here], z_peer[d]),
        )

    def owner_rows(zt, side):
        return pl.ds(pl.multiple_of((2 * zt + side) * owned, 8), owned)

    def to_pair(n):
        sides = [r.outp[n, owner_rows(s, 1 - x), :] for s in range(zs)]
        top = column_top(sides)
        for s in range(zs):
            r.xsend[n, s * owned : (s + 1) * owned, :] = encode(sides[s], top)
        r.xscale_s[n] = top * (1.0 / code_top)
        for copy in x_copies(n):
            copy.start()

    def to_owners(n):
        for copy in x_copies(n):
            copy.wait()
        scale = r.xscale_r[n]
        for s in range(zs):
            part = slice(s * owned, (s + 1) * owned)
            r.ysum[n, part, :] = r.outp[n, owner_rows(s, x), :] + decode(r.xrecv[n, part, :], scale)
        for d in range(1, zs):
            value = r.ysum[n, pl.ds(pl.multiple_of(z_at[d] * owned, 8), owned), :]
            top = column_top([value])
            r.zsend[n, d - 1] = encode(value, top)
            r.zscale_s[n, d - 1] = top * (1.0 / code_top)
            for copy in z_copies(n, d):
                copy.start()

    def finish(n):
        value = r.ysum[n, pl.ds(pl.multiple_of(z * owned, 8), owned), :]
        for d in range(1, zs):
            for copy in z_copies(n, d):
                copy.wait()
            value = value + decode(r.zrecv[n, d - 1], r.zscale_r[n, d - 1])
        at = pl.ds(pl.multiple_of(n * width, width), width)
        r.out[:, at] = r.rsel[:, at] + value * r.tsel[:, at]

    pair_lag, lag = min(2, steps), min(5, steps)

    def step(n, carry):
        both = jnp.dot(r.xbig[...], r.tvm[n], preferred_element_type=jnp.float32)
        r.outp[n] = both[:beliefs] + both[beliefs:]
        to_pair(n)

        @pl.when(n >= pair_lag)
        def _():
            to_owners(n - pair_lag)

        @pl.when(n >= lag)
        def _():
            finish(n - lag)

        return carry

    lax.fori_loop(0, steps, step, 0)
    for n in range(steps - pair_lag, steps):
        to_owners(n)
    for n in range(steps - lag, steps):
        finish(n)
    for copy in sent:
        copy.wait_send()


def fused(alpha_set, transitions, obs_weights, rewards, chosen_idx, chosen_action, groups):
    actions, states = rewards.shape
    obs_local = obs_weights.shape[0]
    beliefs = chosen_action.shape[0]
    ranks = lax.axis_size("obs")
    rows = alpha_set.shape[0]
    cols = states // ranks
    zs, ys = ranks // 2, groups // 2
    sps = cols // lanes
    slabs = zs * sps
    owned = beliefs // ranks
    half_obs = obs_local // 2
    chunks = 8
    chunk = beliefs // chunks
    width = 256
    steps = states // width
    xc = zs * cols
    shared = states // groups
    outer, parts, pairs = max(ys - 1, 1), 2, zs // 2
    plan = (ranks, groups, actions, obs_local, rows, cols, beliefs, chunk, width)
    f32, bf16, i16, i32 = jnp.float32, jnp.bfloat16, jnp.int16, jnp.int32
    vmem, dma = pltpu.VMEM, pltpu.SemaphoreType.DMA
    scratch = dict(
        idx_in=vmem((actions, obs_local, beliefs), i32),
        araw=vmem((groups, rows, xc), bf16),
        aslab=vmem((groups * rows * slabs, lanes), f32),
        wraw=vmem((obs_local, actions, xc), f32),
        w_src=vmem((zs, half_obs, actions, cols), f32),
        w_code_s=vmem((zs, half_obs, actions, cols), i16),
        w_scale_s=vmem((zs, actions, cols), f32),
        w_code=vmem((2, zs, half_obs, actions, cols), i16),
        w_scale=vmem((2, zs, actions, cols), f32),
        wslab=vmem(((2 * obs_local * actions + 1) * slabs, lanes), f32),
        tvm=vmem((steps, actions * cols, width), bf16),
        pick_out=vmem((obs_local, beliefs), i32),
        pick_in=vmem((obs_local, beliefs), i32),
        actb=vmem((beliefs, lanes), i32),
        stage=vmem((slabs * beliefs, lanes), f32),
        totst=vmem((slabs * actions, lanes), f32),
        totrv=vmem((zs - 1, sps * actions, lanes), f32),
        tsum=vmem((sps * actions, lanes), f32),
        psend=vmem((chunks, zs - 1, sps, chunk, lanes), i16),
        precv=vmem((chunks, zs - 1, sps, chunk, lanes), i16),
        pscale_s=vmem((chunks, zs - 1, sps, lanes), f32),
        pscale_r=vmem((chunks, zs - 1, sps, lanes), f32),
        xbig=vmem((2 * beliefs, actions * cols), bf16),
        outp=vmem((steps, beliefs, width), f32),
        ysum=vmem((steps, zs * owned, width), f32),
        xsend=vmem((steps, zs * owned, width), i16),
        xrecv=vmem((steps, zs * owned, width), i16),
        xscale_s=vmem((steps, 1, width), f32),
        xscale_r=vmem((steps, 1, width), f32),
        zsend=vmem((steps, zs - 1, owned, width), i16),
        zrecv=vmem((steps, zs - 1, owned, width), i16),
        zscale_s=vmem((steps, zs - 1, 1, width), f32),
        zscale_r=vmem((steps, zs - 1, 1, width), f32),
        tpart=vmem((actions, shared), f32),
        tz=vmem((zs - 1, actions, shared), f32),
        tx=vmem((2, actions, shared), f32),
        tall=vmem((groups, actions, shared), f32),
        rsel=vmem((owned, states), f32),
        tsel=vmem((owned, states), f32),
        **{f"pick_{k}": pltpu.SMEM((1, beliefs), i32) for k in range(2 * obs_local)},
        pk_l=dma((2 * obs_local + 1,)),
        loc_sem=dma((3, zs)),
        tr_sem=dma((steps,)),
        a_ys=dma((outer, pairs, parts)),
        a_yr=dma((outer, pairs, parts)),
        a_zs=dma((outer, pairs, parts)),
        a_zr=dma((outer, pairs, parts)),
        a_fs=dma((outer, 2, pairs, parts)),
        a_fr=dma((outer, 2, pairs, parts)),
        a_ps=dma((zs,)),
        a_pr=dma((zs,)),
        w_xs=dma((2, zs)),
        w_xr=dma((2, zs)),
        w_fs=dma((2, zs)),
        w_fr=dma((2, zs)),
        pk_s=dma(()),
        pk_r=dma(()),
        tt_zs=dma((zs - 1,)),
        tt_zr=dma((zs - 1,)),
        tt_xs=dma(()),
        tt_xr=dma(()),
        tall_s=dma((groups - 1,)),
        tall_r=dma((groups - 1,)),
        tot_s=dma((zs - 1,)),
        tot_r=dma((zs - 1,)),
        p_s=dma((chunks, zs - 1)),
        p_r=dma((chunks, zs - 1)),
        ps_s=dma((chunks, zs - 1)),
        ps_r=dma((chunks, zs - 1)),
        x_s=dma((steps,)),
        x_r=dma((steps,)),
        xs_s=dma((steps,)),
        xs_r=dma((steps,)),
        z_s=dma((steps, zs - 1)),
        z_r=dma((steps, zs - 1)),
        zs_s=dma((steps, zs - 1)),
        zs_r=dma((steps, zs - 1)),
    )
    hbm = pl.BlockSpec(memory_space=pl.ANY)
    smem = pl.BlockSpec(memory_space=pltpu.SMEM)
    local = pl.BlockSpec(memory_space=pltpu.VMEM)
    names = ("act", "act_row", "rew", "idx", "alpha", "weights", "trans", "out", *scratch)
    return pl.pallas_call(
        functools.partial(fused_kernel, plan, names),
        out_shape=jax.ShapeDtypeStruct((owned, states), f32),
        in_specs=[smem, local, local, hbm, hbm, hbm, hbm],
        out_specs=local,
        scratch_shapes=list(scratch.values()),
        compiler_params=pltpu.CompilerParams(
            collective_id=0, has_side_effects=True, vmem_limit_bytes=67043328
        ),
        name="backup",
    )(
        chosen_action,
        chosen_action[None, :],
        rewards,
        chosen_idx.transpose(1, 2, 0),
        alpha_set,
        obs_weights,
        transitions.reshape(actions * cols, states),
    )


def fits(alpha_set, transitions, obs_weights, beliefs, ranks, groups):
    cols = transitions.shape[1]
    obs_local, actions, states = obs_weights.shape
    return (
        ranks % 4 == 0
        and groups % 2 == 0
        and cols % lanes == 0
        and states == ranks * cols
        and states % (256 * groups) == 0
        and actions % 8 == 0
        and obs_local % 2 == 0
        and alpha_set.shape[0] % 64 == 0
        and beliefs % (16 * ranks) == 0
        and beliefs % 128 == 0
    )


def body(alpha_set, transitions, obs_weights, rewards, chosen_idx, chosen_action):
    actions, states = rewards.shape
    obs_local = obs_weights.shape[0]
    beliefs = chosen_action.shape[0]
    slabs = states // lanes
    ranks = lax.axis_size("obs")
    groups = lax.axis_size("bel")
    if fits(alpha_set, transitions, obs_weights, beliefs, ranks, groups):
        return fused(
            alpha_set, transitions, obs_weights, rewards, chosen_idx, chosen_action, groups
        )
    action_hot = action_table(chosen_action, actions)
    picks = jnp.sum(jnp.where(action_hot[:, :, None] > 0, chosen_idx, 0), axis=1).reshape(-1)
    alpha = lax.all_gather(alpha_set.reshape(-1, slabs, lanes), "bel", axis=0, tiled=True)
    weights = obs_weights.reshape(obs_local * actions, slabs, lanes)
    trans_part = jnp.sum(transitions.astype(jnp.float32), axis=1).reshape(actions, slabs, lanes)
    partial = gather_rows(picks, chosen_action, alpha, weights, trans_part)
    rows = partial.shape[1]
    if slabs % ranks == 0:
        piece = lax.psum_scatter(partial, "obs", scatter_dimension=0, tiled=True)
        piece = piece.transpose(1, 0, 2).reshape(rows, -1)
    else:
        flat = partial.transpose(1, 0, 2).reshape(rows, states)
        piece = lax.psum_scatter(flat, "obs", scatter_dimension=1, tiled=True)
    trans_totals = lax.all_gather(piece[beliefs + actions :], "obs", axis=1, tiled=True)
    moved = move(
        chosen_action, piece[:beliefs], piece[beliefs : beliefs + actions], transitions
    )
    future = lax.psum_scatter(moved, "obs", scatter_dimension=0, tiled=True)
    owned = beliefs // ranks
    own_hot = lax.dynamic_slice_in_dim(action_hot, lax.axis_index("obs") * owned, owned, 0)
    own = functools.partial(
        jnp.dot, own_hot, precision=lax.Precision.HIGHEST, preferred_element_type=jnp.float32
    )
    return own(rewards) + discount * (future / own(trans_totals))


def solution(mesh):
    placed = (
        P("bel", None),
        P(None, "obs", None),
        P("obs", None, None),
        P(),
        P("bel", None, "obs"),
        P("bel"),
    )
    return jax.shard_map(
        body, mesh=mesh, in_specs=placed, out_specs=P(("bel", "obs"), None), check_vma=False
    )
```

```python
import functools
import types

import jax
import jax.numpy as jnp
from jax import lax
from jax.experimental import pallas as pl
from jax.experimental.pallas import tpu as pltpu
from jax.sharding import PartitionSpec as P

discount = 0.95
lanes = 128


def gather_kernel(picks_ref, act_ref, alpha_ref, weights_ref, moves_ref, out_ref):
    beliefs = act_ref.shape[0]
    obs_local = picks_ref.shape[0] // beliefs
    actions = weights_ref.shape[0] // obs_local
    slabs = alpha_ref.shape[1]
    rows = out_ref.shape[0] // slabs

    def one(b, carry):
        action = act_ref[b]
        sums = [None] * min(4, obs_local)
        for o in range(obs_local):
            row = alpha_ref[picks_ref[b * obs_local + o]].astype(jnp.float32)
            term = row * weights_ref[o * actions + action]
            at = o % len(sums)
            sums[at] = term if sums[at] is None else sums[at] + term
        out_ref[pl.ds(b, slabs, stride=rows), :] = functools.reduce(jnp.add, sums)
        return carry

    lax.fori_loop(0, beliefs, one, 0)

    def total(a, carry):
        acc = weights_ref[a]
        for o in range(1, obs_local):
            acc = acc + weights_ref[o * actions + a]
        out_ref[pl.ds(beliefs + a, slabs, stride=rows), :] = acc
        out_ref[pl.ds(beliefs + actions + a, slabs, stride=rows), :] = moves_ref[a]
        return carry

    lax.fori_loop(0, actions, total, 0)


def gather_rows(picks, acts, alpha, weights, moves):
    slabs = alpha.shape[1]
    beliefs = acts.shape[0]
    rows = beliefs + 2 * moves.shape[0]
    vmem = pl.BlockSpec(memory_space=pltpu.VMEM)
    smem = pl.BlockSpec(memory_space=pltpu.SMEM)
    out = pl.pallas_call(
        gather_kernel,
        out_shape=jax.ShapeDtypeStruct((slabs * rows, lanes), jnp.float32),
        in_specs=[smem, smem, vmem, vmem, vmem],
        out_specs=vmem,
        compiler_params=pltpu.CompilerParams(vmem_limit_bytes=40 << 20),
        cost_estimate=pl.CostEstimate(
            flops=80_000_000, bytes_accessed=16 << 20, transcendentals=0
        ),
        name="gather_rows",
    )(picks, acts, alpha, weights, moves)
    return out.reshape(slabs, rows, lanes)


def move_kernel(act_ref, w_ref, tot_ref, table_ref, out_ref):
    a = pl.program_id(0)
    scaled = w_ref[...] / tot_ref[0]
    x = jnp.where(act_ref[...] == a, scaled, 0.0)
    high = x.astype(jnp.bfloat16)
    low = (x - high.astype(jnp.float32)).astype(jnp.bfloat16)
    table = table_ref[0]
    both = jnp.dot(jnp.concatenate([high, low], axis=0), table, preferred_element_type=jnp.float32)
    half = x.shape[0]
    part = both[:half] + both[half:]

    @pl.when(a == 0)
    def _():
        out_ref[...] = part

    @pl.when(a > 0)
    def _():
        out_ref[...] += part


def move(acts, weighted, totals, table):
    beliefs, width = weighted.shape
    actions, _, states = table.shape
    return pl.pallas_call(
        move_kernel,
        grid=(actions,),
        out_shape=jax.ShapeDtypeStruct((beliefs, states), jnp.float32),
        in_specs=[
            pl.BlockSpec((beliefs, 1), lambda a: (0, 0)),
            pl.BlockSpec((beliefs, width), lambda a: (0, 0)),
            pl.BlockSpec((1, 1, width), lambda a: (a, 0, 0)),
            pl.BlockSpec((1, width, states), lambda a: (a, 0, 0)),
        ],
        out_specs=pl.BlockSpec((beliefs, states), lambda a: (0, 0)),
        compiler_params=pltpu.CompilerParams(
            vmem_limit_bytes=48 << 20, dimension_semantics=("arbitrary",)
        ),
        cost_estimate=pl.CostEstimate(
            flops=4 * beliefs * width * actions * states,
            bytes_accessed=2 * actions * width * states,
            transcendentals=0,
        ),
        name="move",
    )(acts[:, None], weighted, totals[:, None, :], table)


def action_table(actions, count):
    return (actions[:, None] == jnp.arange(count, dtype=jnp.int32)[None, :]).astype(jnp.float32)


MESH = pl.DeviceIdType.MESH
code_top = 32767.0


def encode(values, top):
    q = (values * (code_top / top) + (code_top + 1.5)).astype(jnp.int32) - 32768
    return q.astype(jnp.int16)


def column_top(blocks):
    tops = [jnp.max(jnp.abs(v), axis=0, keepdims=True) for v in blocks]
    return jnp.maximum(functools.reduce(jnp.maximum, tops), 1e-30)


def decode(codes, scale):
    return codes.astype(jnp.int32).astype(jnp.float32) * scale


def fused_kernel(plan, names, *refs):
    r = types.SimpleNamespace(**dict(zip(names, refs)))
    ranks, groups, actions, obs_local, rows, cols, beliefs, parts_of, width = plan
    zs, ys = ranks // 2, groups // 2
    sps = cols // lanes
    slabs = zs * sps
    owned = beliefs // ranks
    half_obs = obs_local // 2
    chunk, tail = parts_of
    first_rows = ranks * chunk
    counts = (ranks, ranks * tail // chunk)
    steps = zs * 2 * cols // width
    share = steps // groups
    parts = r.a_yr.shape[2]
    part_rows = rows // parts
    pairs = zs // 2

    me_o, me_b = lax.axis_index("obs"), lax.axis_index("bel")
    z, x = lax.div(me_o, 2), lax.rem(me_o, 2)
    y, c = lax.div(me_b, 2), lax.rem(me_b, 2)
    odd = lax.rem(z, 2)
    other = me_b + 1 - 2 * c
    x_peer = {"obs": me_o + 1 - 2 * x}
    core_peer = {"bel": other}
    next_z = {"obs": (z + 1 - 2 * odd) * 2 + x}
    z_at = [lax.rem(z + d, zs) for d in range(zs)]
    z_peer = [{"obs": zt * 2 + x} for zt in z_at]
    y_peer = [{"bel": lax.rem(y + d, ys) * 2 + c} for d in range(ys)]
    y_from = [lax.rem(y + ys - d, ys) for d in range(ys)]
    b_peer = [{"bel": lax.rem(me_b + d, groups)} for d in range(groups)]
    b_from = [lax.rem(me_b + groups - d, groups) for d in range(groups)]

    def remote(src, dst, s_sem, r_sem, where):
        return pltpu.make_async_remote_copy(
            src_ref=src,
            dst_ref=dst,
            send_sem=s_sem,
            recv_sem=r_sem,
            device_id=where,
            device_id_type=MESH,
        )

    def drain_sends(ref, sem):
        remote(ref, ref, sem, sem, x_peer).wait_send()

    def drain_receives(ref, sem):
        remote(ref, ref, sem, sem, x_peer).wait_recv()

    def drain_local(ref, sem):
        pltpu.make_async_copy(ref, ref, sem).wait()

    def band(s):
        return pl.ds(pl.multiple_of(s * cols, lanes), cols)

    def source_band(s, side):
        return pl.ds(pl.multiple_of((2 * s + side) * cols, lanes), cols)

    def half(side):
        return pl.ds(side * half_obs, half_obs)

    own_idx = pltpu.make_async_copy(r.idx, r.idx_in, r.idx_sem)
    peer_w = [
        pltpu.make_async_copy(
            r.weights.at[half(c), :, source_band(s, 1 - x)], r.w_src.at[s], r.loc_sem.at[s]
        )
        for s in range(zs)
    ]
    own_w = [
        pltpu.make_async_copy(
            r.weights.at[:, :, source_band(s, x)], r.wraw.at[:, :, band(s)], r.ow_sem
        )
        for s in range(zs)
    ]
    own_a = [
        pltpu.make_async_copy(
            r.alpha.at[:, source_band(s, x)], r.araw.at[me_b, :, band(s)], r.oa_sem
        )
        for s in range(zs)
    ]
    table = []
    for k in range(steps):
        n = lax.rem(me_b * share + k, steps)
        at = pl.ds(pl.multiple_of(n * width, lanes), width)
        table.append(pltpu.make_async_copy(r.trans.at[:, at], r.tvm.at[n], r.tr_sem.at[min(k, share)]))
    for copy in peer_w + [own_idx] + own_w + table[:share] + own_a + table[share:]:
        copy.start()

    peers = [x_peer] + z_peer[1:] + b_peer[1:]
    barrier = pltpu.get_barrier_semaphore()
    for peer in peers:
        pl.semaphore_signal(barrier, inc=1, device_id=peer, device_id_type=MESH)
    pl.semaphore_wait(barrier, len(peers))

    def rows_of(h):
        return pl.ds(h * part_rows, part_rows)

    def near(k):
        return 2 * k + odd

    def far(k):
        return 2 * k + 1 - odd

    pieces = [(k, h) for k in range(pairs) for h in range(parts)]
    def launch(copy):
        copy.start()

    for k, h in pieces:
        for d in range(1, ys):
            launch(
                remote(
                    r.alpha.at[rows_of(h), source_band(near(k), x)],
                    r.araw.at[me_b, rows_of(h), band(near(k))],
                    r.a_ys.at[d - 1],
                    r.a_yr.at[d - 1, k, h],
                    y_peer[d],
                )
            )
    a_core = [
        remote(
            r.alpha.at[:, source_band(s, x)],
            r.araw.at[me_b, :, band(s)],
            r.a_ps,
            r.a_pr,
            core_peer,
        )
        for s in range(zs)
    ]
    for copy in a_core:
        launch(copy)

    w_out = []
    for s in range(zs):
        peer_w[s].wait()
        for at in range(0, cols, lanes):
            value = r.w_src[s, :, :, at : at + lanes]
            top = jnp.maximum(jnp.max(jnp.abs(value), axis=0), 1e-30)
            r.w_code_s[s, :, :, at : at + lanes] = encode(value, top[None])
            r.w_scale_s[s, :, at : at + lanes] = top * (1.0 / code_top)
        w_out.append(
            (
                remote(r.w_code_s.at[s], r.w_code.at[c, s], r.w_xs.at[0], r.w_xr.at[0, s], x_peer),
                remote(
                    r.w_scale_s.at[s], r.w_scale.at[c, s], r.w_xs.at[1], r.w_xr.at[1, s], x_peer
                ),
            )
        )
        for copy in w_out[-1]:
            launch(copy)

    pick_sm = [getattr(r, f"pick_{k}") for k in range(2 * obs_local)]

    def store_picks(source, first):
        for o in range(obs_local):
            pltpu.make_async_copy(
                source.at[pl.ds(o, 1), :], pick_sm[first + o], r.pk_l.at[first // obs_local]
            ).start()

    def own_picks():
        own_idx.wait()
        action_row = r.act_row[...].reshape(1, beliefs)
        chosen = jnp.zeros((obs_local, beliefs), jnp.int32)
        for a in range(actions):
            chosen = jnp.where(action_row == a, r.idx_in[a], chosen)
        r.pick_out[...] = chosen * slabs

    pick_copy = remote(r.pick_out, r.pick_in, r.pk_s, r.pk_r, x_peer)
    tt_out = [
        remote(r.tpart, r.tz.at[d - 1], r.tt_zs, r.tt_zr, z_peer[d])
        for d in range(1, zs)
    ]
    tx_out = remote(r.tx.at[0], r.tx.at[1], r.tt_xs, r.tt_xr, x_peer)

    def transition_totals():
        for k in range(share):
            table[k].wait()
            n = me_b * share + k

            def column_total(a, carry, n=n, k=k):
                value = r.tvm[n, pl.ds(pl.multiple_of(a * cols, 16), cols), :].astype(jnp.float32)
                r.tpart[pl.ds(a, 1), k * width : (k + 1) * width] = jnp.sum(
                    value, axis=0, keepdims=True
                )
                return carry

            lax.fori_loop(0, actions, column_total, 0)

    def action_lanes(owner, carry):
        for k in range(owned):
            at = owner * chunk + k if k < chunk else first_rows + owner * tail + k - chunk
            r.actb[pl.ds(at, 1), :] = jnp.full((1, lanes), r.act[owner * owned + k], jnp.int32)
        return carry

    pad = slabs

    def own_weight_slab(s):
        def one(o, carry):
            for h in range(sps):
                at = s * cols + h * lanes
                first = o * actions * slabs + s * sps + h + pad
                r.wslab[pl.ds(first, actions, stride=slabs), :] = r.wraw[o, :, at : at + lanes]
            return carry

        lax.fori_loop(0, obs_local, one, 0)

    def peer_weight_slab(side, s):
        def one(o, carry):
            for h in range(sps):
                at = slice(h * lanes, (h + 1) * lanes)
                first = (obs_local + side * half_obs + o) * actions * slabs + s * sps + h + pad
                r.wslab[pl.ds(first, actions, stride=slabs), :] = decode(
                    r.w_code[side, s, o, :, at], r.w_scale[side, s, :, at]
                )
            return carry

        lax.fori_loop(0, half_obs, one, 0)

    def alpha_slab(member, s, first_row, count):
        def one(i, carry):
            for k in range(2):
                r0 = pl.multiple_of(first_row + i * 32 + k * 16, 16)
                for h in range(sps):
                    at = pl.ds(pl.multiple_of(s * cols + h * lanes, lanes), lanes)
                    first = (member * rows + r0) * slabs + s * sps + h
                    r.aslab[pl.ds(first, 16, stride=slabs), :] = r.araw[
                        member, pl.ds(r0, 16), at
                    ].astype(jnp.float32)
            return carry

        lax.fori_loop(0, count // 32, one, 0)

    late = []

    def arrived(k, h, by_z):
        s = far(k) if by_z else near(k)
        for d in range(1, ys):
            member = y_from[d] * 2 + c
            slot = r.araw.at[member, rows_of(h), band(s)]
            here = (d - 1, k, h)
            if by_z:
                drain_receives(slot, r.a_zr.at[here])
            else:
                drain_receives(slot, r.a_yr.at[here])
                launch(remote(slot, slot, r.a_zs.at[d - 1], r.a_zr.at[here], next_z))
            at = (d - 1, int(by_z), k, h)
            forward = remote(slot, slot, r.a_fs.at[d - 1], r.a_fr.at[at], core_peer)
            launch(forward)
            alpha_slab(member, s, h * part_rows, part_rows)

            def rest(forward=forward, member=y_from[d] * 2 + 1 - c):
                forward.wait_recv()
                alpha_slab(member, s, h * part_rows, part_rows)

            late.append(rest)

    def weights_arrived(s):
        both = []
        for k, copy in enumerate(w_out[s]):
            copy.wait_recv()
            held = (r.w_code, r.w_scale)[k].at[c, s]
            both.append(remote(held, held, r.w_fs.at[k], r.w_fr.at[k, s], core_peer))
            launch(both[-1])
        peer_weight_slab(c, s)

        def rest():
            for copy in both:
                copy.wait_recv()
            peer_weight_slab(1 - c, s)

        late.append(rest)

    own_picks()
    pick_copy.start()
    store_picks(r.pick_out, 0)
    drain_local(r.wraw, r.ow_sem)
    for s in range(zs):
        own_weight_slab(s)
    drain_local(r.araw.at[me_b], r.oa_sem)
    for s in range(zs):
        alpha_slab(me_b, s, 0, rows)
    count = len(pieces)
    for i in range(count + 1):
        ready, late = late, []
        if i < count:
            arrived(*pieces[i], False)
        if i >= 1:
            arrived(*pieces[i - 1], True)
        for s in range(i * zs // (count + 1), (i + 1) * zs // (count + 1)):
            weights_arrived(s)
        for rest in ready:
            rest()
        if i == 0:
            transition_totals()
            for copy in tt_out:
                copy.start()
        if i == 1:
            drain_receives(r.araw.at[other], r.a_pr)
            for s in range(zs):
                alpha_slab(other, s, 0, rows)
        if i == 2:
            pick_copy.wait()
            store_picks(r.pick_in, obs_local)
    for rest in late:
        rest()
    drain_sends(r.tz, r.tt_zs)
    drain_receives(r.tz, r.tt_zr)
    total = r.tpart[...]
    for d in range(1, zs):
        total = total + r.tz[d - 1]
    r.tx[0] = total

    def obs_total(a, carry):
        sums = [None] * 4
        for o in range(2 * obs_local):
            term = r.wslab[pl.ds(pl.multiple_of((o * actions + a) * slabs + pad, slabs), slabs), :]
            sums[o % 4] = term if sums[o % 4] is None else sums[o % 4] + term
        r.totst[pl.ds(a, slabs, stride=actions), :] = (sums[0] + sums[1]) + (sums[2] + sums[3])
        return carry

    lax.fori_loop(0, actions, obs_total, 0)
    tot_rows = sps * actions
    tot_out = [
        remote(
            r.totst.at[pl.ds(pl.multiple_of(z_at[d] * tot_rows, 8), tot_rows)],
            r.totrv.at[d - 1],
            r.tot_s,
            r.tot_r,
            z_peer[d],
        )
        for d in range(1, zs)
    ]
    tall_out = [
        remote(
            r.tall.at[me_b], r.tall.at[me_b], r.tall_s, r.tall_r, b_peer[d]
        )
        for d in range(1, groups)
    ]
    for copy in tot_out + [tx_out]:
        copy.start()
    drain_local(r.pick_out, r.pk_l.at[0])
    drain_local(r.pick_in, r.pk_l.at[1])

    def share_totals():
        tx_out.wait()
        r.tall[me_b] = r.tx[0] + r.tx[1]
        for copy in tall_out:
            copy.start()

    def p_copies(q, d):
        here = (q, d - 1)
        return (
            remote(r.psend.at[here], r.precv.at[here], r.p_s, r.p_r.at[q], z_peer[d]),
            remote(
                r.pscale_s.at[here], r.pscale_r.at[here], r.ps_s, r.ps_r.at[q], z_peer[d]
            ),
        )

    unroll = 4

    def gather_chunk(q, part):
        def one(i, carry):
            if part == 0:
                b0 = q * owned + i * unroll
            else:
                row = i * unroll
                owner = (q - ranks) * (chunk // tail) + lax.div(row, tail)
                b0 = owner * owned + chunk + lax.rem(row, tail)
            for t in range(unroll):
                b = b0 + t
                base = r.act[b] * slabs
                sums = [None] * 4
                for p in range(2):
                    for o in range(obs_local):
                        row = r.aslab[pl.ds(pick_sm[p * obs_local + o][0, b], slabs), :]
                        at = (p * obs_local + o) * actions * slabs + pad
                        term = row * r.wslab[pl.ds(base + at, slabs), :]
                        k = o % 4
                        sums[k] = term if sums[k] is None else sums[k] + term
                r.stage[pl.ds(q * chunk + i * unroll + t, slabs, stride=beliefs), :] = (sums[0] + sums[1]) + (
                    sums[2] + sums[3]
                )
            return carry

        lax.fori_loop(0, chunk // unroll, one, 0)
        for d in range(1, zs):
            for h in range(sps):
                first = (z_at[d] * sps + h) * beliefs + q * chunk
                value = r.stage[pl.ds(pl.multiple_of(first, 8), chunk), :]
                top = column_top([value])
                r.psend[q, d - 1, h] = encode(value, top)
                r.pscale_s[q, d - 1, h : h + 1, :] = top * (1.0 / code_top)
            for copy in p_copies(q, d):
                copy.start()

    def prepare():
        drain_sends(r.totrv, r.tot_s)
        drain_receives(r.totrv, r.tot_r)
        drain_sends(r.tall.at[pl.ds(0, groups - 1)], r.tall_s)
        drain_receives(r.tall.at[pl.ds(0, groups - 1)], r.tall_r)
        totals = r.totst[pl.ds(pl.multiple_of(z * tot_rows, 8), tot_rows), :]
        for d in range(1, zs):
            totals = totals + r.totrv[d - 1]
        r.tsum[...] = totals
        own_act = jnp.concatenate(
            [
                r.actb[pl.ds(pl.multiple_of(me_o * chunk, 8), chunk), :],
                r.actb[pl.ds(pl.multiple_of(first_rows + me_o * tail, 8), tail), :],
            ],
            axis=0,
        )
        per_member = share * width // lanes

        for member in range(groups):
            for k in range(per_member):
                at = slice(k * lanes, (k + 1) * lanes)
                to = slice((member * per_member + k) * lanes, (member * per_member + k + 1) * lanes)
                reward = jnp.zeros((owned, lanes), jnp.float32)
                scale = jnp.ones((owned, lanes), jnp.float32)
                for a in range(actions):
                    hit = own_act == a
                    reward = jnp.where(hit, r.rew[a : a + 1, to], reward)
                    scale = jnp.where(hit, r.tall[member, a : a + 1, at], scale)
                r.rsel[:, to] = reward
                r.tsel[:, to] = discount / scale

    def absorb(q, part):
        drain_receives(r.precv.at[q], r.p_r.at[q])
        drain_receives(r.pscale_r.at[q], r.ps_r.at[q])
        b0 = pl.multiple_of(q * chunk, 16)
        into = (r.xbig0, r.xbig1)[part]
        at_row = pl.multiple_of(q * chunk - part * first_rows, 16)
        at_low = pl.multiple_of(at_row + into.shape[0] // 2, 16)
        act = r.actb[pl.ds(b0, chunk), :]
        for h in range(sps):
            first = (z * sps + h) * beliefs + q * chunk
            value = r.stage[pl.ds(pl.multiple_of(first, 8), chunk), :]
            for d in range(1, zs):
                value = value + decode(r.precv[q, d - 1, h], r.pscale_r[q, d - 1, h : h + 1, :])
            under = jnp.ones_like(value)
            for a in range(actions):
                at = h * actions + a
                under = jnp.where(act == a, r.tsum[at : at + 1, :], under)
            value = value / under
            high = value.astype(jnp.bfloat16).astype(jnp.float32)
            low = value - high
            for a in range(actions):
                at = slice(a * cols + h * lanes, a * cols + (h + 1) * lanes)
                hit = act == a
                into[pl.ds(at_row, chunk), at] = jnp.where(hit, high, 0.0).astype(jnp.bfloat16)
                into[pl.ds(at_low, chunk), at] = jnp.where(hit, low, 0.0).astype(jnp.bfloat16)

    behind = 3

    def gather_first(q, carry):
        gather_chunk(q, 0)

        @pl.when(q == 0)
        def _():
            share_totals()

        @pl.when(q == behind - 1)
        def _():
            prepare()

        @pl.when(q >= behind)
        def _():
            absorb(q - behind, 0)

        return carry

    def gather_last(j, carry):
        gather_chunk(ranks + j, 1)

        @pl.when(j < behind)
        def _():
            absorb(ranks - behind + j, 0)

        return carry

    lax.fori_loop(0, ranks, action_lanes, 0)
    lax.fori_loop(0, counts[0], gather_first, 0)
    lax.fori_loop(0, counts[1], gather_last, 0)
    drain_local(r.tvm.at[pl.ds(0, steps - share)], r.tr_sem.at[share])

    sizes = (chunk, tail)
    sets = [
        types.SimpleNamespace(
            **{name: getattr(r, name + str(part)) for name in part_names}, rows=sizes[part]
        )
        for part in range(2)
    ]

    def x_copies(part, n):
        t, here = sets[part], (part, n)
        return (
            remote(t.xsend.at[n], t.xrecv.at[n], r.x_s.at[part], r.x_r.at[here], x_peer),
            remote(t.xscale_s.at[n], t.xscale_r.at[n], r.xs_s.at[part], r.xs_r.at[here], x_peer),
        )

    def z_copies(part, n, d):
        t, here, k = sets[part], (part, n), (n, d - 1)
        return (
            remote(t.zsend.at[k], t.zrecv.at[k], r.z_s.at[part], r.z_r.at[here], z_peer[d]),
            remote(
                t.zscale_s.at[k], t.zscale_r.at[k], r.zs_s.at[part], r.zs_r.at[here], z_peer[d]
            ),
        )

    def product(part, n):
        t = sets[part]
        both = jnp.dot(t.xbig[...], r.tvm[n], preferred_element_type=jnp.float32)
        count = both.shape[0] // 2
        t.outp[n] = both[:count] + both[count:]
        owner = [
            t.outp[n, pl.ds(pl.multiple_of((2 * s + 1 - x) * t.rows, 8), t.rows), :]
            for s in range(zs)
        ]
        top = column_top(owner)
        for s in range(zs):
            t.xsend[n, s * t.rows : (s + 1) * t.rows, :] = encode(owner[s], top)
        t.xscale_s[n] = top * (1.0 / code_top)
        for copy in x_copies(part, n):
            copy.start()

    def to_owners(part, n):
        t = sets[part]
        for copy in x_copies(part, n):
            copy.wait_recv()
        scale = t.xscale_r[n]
        for s in range(zs):
            at = slice(s * t.rows, (s + 1) * t.rows)
            kept = t.outp[n, pl.ds(pl.multiple_of((2 * s + x) * t.rows, 8), t.rows), :]
            t.ysum[n, at, :] = kept + decode(t.xrecv[n, at, :], scale)
        for d in range(1, zs):
            value = t.ysum[n, pl.ds(pl.multiple_of(z_at[d] * t.rows, 8), t.rows), :]
            top = column_top([value])
            t.zsend[n, d - 1] = encode(value, top)
            t.zscale_s[n, d - 1] = top * (1.0 / code_top)
            for copy in z_copies(part, n, d):
                copy.start()

    def finish(part, n):
        t = sets[part]
        value = t.ysum[n, pl.ds(pl.multiple_of(z * t.rows, 8), t.rows), :]
        drain_receives(t.zrecv.at[n], r.z_r.at[part, n])
        drain_receives(t.zscale_r.at[n], r.zs_r.at[part, n])
        for d in range(1, zs):
            value = value + decode(t.zrecv[n, d - 1], t.zscale_r[n, d - 1])
        at = pl.ds(pl.multiple_of(n * width, width), width)
        to = slice(part * chunk, part * chunk + t.rows)
        r.out[to, at] = r.rsel[to, at] + value * r.tsel[to, at]

    lag = min(3, steps)

    def first_step(n, carry):
        product(0, n)

        @pl.when(n >= lag)
        def _():
            to_owners(0, n - lag)

        @pl.when(n >= steps - counts[1])
        def _():
            absorb(ranks + n - (steps - counts[1]), 1)

        return carry

    def last_step(n, carry):
        product(1, n)

        @pl.when(n < lag)
        def _():
            to_owners(0, n + steps - lag)

        @pl.when(n >= lag)
        def _():
            to_owners(1, n - lag)

        finish(0, n)
        return carry

    lax.fori_loop(0, steps, first_step, 0)
    lax.fori_loop(0, steps, last_step, 0)
    for n in range(steps - lag, steps):
        to_owners(1, n)
    for n in range(steps):
        finish(1, n)
    for part, t in enumerate(sets):
        drain_sends(t.xsend, r.x_s.at[part])
        drain_sends(t.xscale_s, r.xs_s.at[part])
        drain_sends(t.zsend, r.z_s.at[part])
        drain_sends(t.zscale_s, r.zs_s.at[part])
    drain_sends(r.psend, r.p_s)
    drain_sends(r.pscale_s, r.ps_s)
    drain_sends(r.w_code_s, r.w_xs.at[0])
    drain_sends(r.w_scale_s, r.w_xs.at[1])
    drain_sends(r.w_code.at[0], r.w_fs.at[0])
    drain_sends(r.w_scale.at[0], r.w_fs.at[1])
    drain_sends(r.araw.at[0], r.a_ps)
    for d in range(1, ys):
        drain_sends(r.araw.at[0, :, pl.ds(0, pairs * cols)], r.a_ys.at[d - 1])
        drain_sends(r.araw.at[0, :, pl.ds(0, pairs * cols)], r.a_zs.at[d - 1])
        drain_sends(r.araw.at[0], r.a_fs.at[d - 1])


part_names = (
    "xbig",
    "outp",
    "ysum",
    "xsend",
    "xrecv",
    "xscale_s",
    "xscale_r",
    "zsend",
    "zrecv",
    "zscale_s",
    "zscale_r",
)


def fused(alpha_set, transitions, obs_weights, rewards, chosen_idx, chosen_action, groups):
    actions, states = rewards.shape
    obs_local = obs_weights.shape[0]
    beliefs = chosen_action.shape[0]
    ranks = lax.axis_size("obs")
    rows = alpha_set.shape[0]
    cols = states // ranks
    zs, ys = ranks // 2, groups // 2
    sps = cols // lanes
    slabs = zs * sps
    owned = beliefs // ranks
    half_obs = obs_local // 2
    tail = 16
    chunk = owned - tail
    chunks = ranks + ranks * tail // chunk
    width = 256
    steps = states // width
    xc = zs * cols
    shared = states // groups
    outer, parts, pairs = max(ys - 1, 1), 2, zs // 2
    plan = (ranks, groups, actions, obs_local, rows, cols, beliefs, (chunk, tail), width)
    f32, bf16, i16, i32 = jnp.float32, jnp.bfloat16, jnp.int16, jnp.int32
    vmem, dma = pltpu.VMEM, pltpu.SemaphoreType.DMA
    scratch = dict(
        idx_in=vmem((actions, obs_local, beliefs), i32),
        araw=vmem((groups, rows, xc), bf16),
        aslab=vmem((groups * rows * slabs, lanes), f32),
        wraw=vmem((obs_local, actions, xc), f32),
        w_src=vmem((zs, half_obs, actions, cols), f32),
        w_code_s=vmem((zs, half_obs, actions, cols), i16),
        w_scale_s=vmem((zs, actions, cols), f32),
        w_code=vmem((2, zs, half_obs, actions, cols), i16),
        w_scale=vmem((2, zs, actions, cols), f32),
        wslab=vmem(((2 * obs_local * actions + 1) * slabs, lanes), f32),
        tvm=vmem((steps, actions * cols, width), bf16),
        pick_out=vmem((obs_local, beliefs), i32),
        pick_in=vmem((obs_local, beliefs), i32),
        actb=vmem((beliefs, lanes), i32),
        stage=vmem((slabs * beliefs, lanes), f32),
        totst=vmem((slabs * actions, lanes), f32),
        totrv=vmem((zs - 1, sps * actions, lanes), f32),
        tsum=vmem((sps * actions, lanes), f32),
        psend=vmem((chunks, zs - 1, sps, chunk, lanes), i16),
        precv=vmem((chunks, zs - 1, sps, chunk, lanes), i16),
        pscale_s=vmem((chunks, zs - 1, sps, lanes), f32),
        pscale_r=vmem((chunks, zs - 1, sps, lanes), f32),
        tpart=vmem((actions, shared), f32),
        tz=vmem((zs - 1, actions, shared), f32),
        tx=vmem((2, actions, shared), f32),
        tall=vmem((groups, actions, shared), f32),
        rsel=vmem((owned, states), f32),
        tsel=vmem((owned, states), f32),
        **{f"pick_{k}": pltpu.SMEM((1, beliefs), i32) for k in range(2 * obs_local)},
        pk_l=dma((2,)),
        idx_sem=dma(()),
        ow_sem=dma(()),
        oa_sem=dma(()),
        loc_sem=dma((zs,)),
        tr_sem=dma((steps // groups + 1,)),
        a_ys=dma((outer,)),
        a_yr=dma((outer, pairs, parts)),
        a_zs=dma((outer,)),
        a_zr=dma((outer, pairs, parts)),
        a_fs=dma((outer,)),
        a_fr=dma((outer, 2, pairs, parts)),
        a_ps=dma(()),
        a_pr=dma(()),
        w_xs=dma((2,)),
        w_xr=dma((2, zs)),
        w_fs=dma((2,)),
        w_fr=dma((2, zs)),
        pk_s=dma(()),
        pk_r=dma(()),
        tt_zs=dma(()),
        tt_zr=dma(()),
        tt_xs=dma(()),
        tt_xr=dma(()),
        tall_s=dma(()),
        tall_r=dma(()),
        tot_s=dma(()),
        tot_r=dma(()),
        p_s=dma(()),
        p_r=dma((chunks,)),
        ps_s=dma(()),
        ps_r=dma((chunks,)),
        x_s=dma((2,)),
        x_r=dma((2, steps)),
        xs_s=dma((2,)),
        xs_r=dma((2, steps)),
        z_s=dma((2,)),
        z_r=dma((2, steps)),
        zs_s=dma((2,)),
        zs_r=dma((2, steps)),
    )
    for part, count in enumerate((chunk, tail)):
        shapes = (
            vmem((2 * ranks * count, actions * cols), bf16),
            vmem((steps, ranks * count, width), f32),
            vmem((steps, zs * count, width), f32),
            vmem((steps, zs * count, width), i16),
            vmem((steps, zs * count, width), i16),
            vmem((steps, 1, width), f32),
            vmem((steps, 1, width), f32),
            vmem((steps, zs - 1, count, width), i16),
            vmem((steps, zs - 1, count, width), i16),
            vmem((steps, zs - 1, 1, width), f32),
            vmem((steps, zs - 1, 1, width), f32),
        )
        scratch.update(zip([name + str(part) for name in part_names], shapes))
    hbm = pl.BlockSpec(memory_space=pl.ANY)
    smem = pl.BlockSpec(memory_space=pltpu.SMEM)
    local = pl.BlockSpec(memory_space=pltpu.VMEM)
    names = ("act", "act_row", "rew", "idx", "alpha", "weights", "trans", "out", *scratch)
    return pl.pallas_call(
        functools.partial(fused_kernel, plan, names),
        out_shape=jax.ShapeDtypeStruct((owned, states), f32),
        in_specs=[smem, local, local, hbm, hbm, hbm, hbm],
        out_specs=local,
        scratch_shapes=list(scratch.values()),
        compiler_params=pltpu.CompilerParams(
            collective_id=0, has_side_effects=True, vmem_limit_bytes=67043328
        ),
        name="backup",
    )(
        chosen_action,
        chosen_action,
        rewards,
        chosen_idx.transpose(1, 2, 0),
        alpha_set,
        obs_weights,
        transitions.reshape(actions * cols, states),
    )


def fits(alpha_set, transitions, obs_weights, beliefs, ranks, groups):
    cols = transitions.shape[1]
    obs_local, actions, states = obs_weights.shape
    return (
        ranks % 4 == 0
        and groups % 2 == 0
        and cols % lanes == 0
        and states == ranks * cols
        and states % (256 * groups) == 0
        and actions % 8 == 0
        and obs_local % 2 == 0
        and alpha_set.shape[0] % 64 == 0
        and beliefs % (16 * ranks) == 0
        and beliefs > 16 * ranks
        and ranks * 16 % (beliefs // ranks - 16) == 0
        and ranks * 16 // (beliefs // ranks - 16) <= states // 256
        and ranks * 16 // (beliefs // ranks - 16) >= 3
    )


def body(alpha_set, transitions, obs_weights, rewards, chosen_idx, chosen_action):
    actions, states = rewards.shape
    obs_local = obs_weights.shape[0]
    beliefs = chosen_action.shape[0]
    slabs = states // lanes
    ranks = lax.axis_size("obs")
    groups = lax.axis_size("bel")
    if fits(alpha_set, transitions, obs_weights, beliefs, ranks, groups):
        return fused(
            alpha_set, transitions, obs_weights, rewards, chosen_idx, chosen_action, groups
        )
    action_hot = action_table(chosen_action, actions)
    picks = jnp.sum(jnp.where(action_hot[:, :, None] > 0, chosen_idx, 0), axis=1).reshape(-1)
    alpha = lax.all_gather(alpha_set.reshape(-1, slabs, lanes), "bel", axis=0, tiled=True)
    weights = obs_weights.reshape(obs_local * actions, slabs, lanes)
    trans_part = jnp.sum(transitions.astype(jnp.float32), axis=1).reshape(actions, slabs, lanes)
    partial = gather_rows(picks, chosen_action, alpha, weights, trans_part)
    rows = partial.shape[1]
    if slabs % ranks == 0:
        piece = lax.psum_scatter(partial, "obs", scatter_dimension=0, tiled=True)
        piece = piece.transpose(1, 0, 2).reshape(rows, -1)
    else:
        flat = partial.transpose(1, 0, 2).reshape(rows, states)
        piece = lax.psum_scatter(flat, "obs", scatter_dimension=1, tiled=True)
    trans_totals = lax.all_gather(piece[beliefs + actions :], "obs", axis=1, tiled=True)
    moved = move(
        chosen_action, piece[:beliefs], piece[beliefs : beliefs + actions], transitions
    )
    future = lax.psum_scatter(moved, "obs", scatter_dimension=0, tiled=True)
    owned = beliefs // ranks
    own_hot = lax.dynamic_slice_in_dim(action_hot, lax.axis_index("obs") * owned, owned, 0)
    own = functools.partial(
        jnp.dot, own_hot, precision=lax.Precision.HIGHEST, preferred_element_type=jnp.float32
    )
    return own(rewards) + discount * (future / own(trans_totals))


def solution(mesh):
    placed = (
        P("bel", None),
        P(None, "obs", None),
        P("obs", None, None),
        P(),
        P("bel", None, "obs"),
        P("bel"),
    )
    return jax.shard_map(
        body, mesh=mesh, in_specs=placed, out_specs=P(("bel", "obs"), None), check_vma=False
    )
```

```python
import functools
import types

import jax
import jax.numpy as jnp
from jax import lax
from jax.experimental import pallas as pl
from jax.experimental.pallas import tpu as pltpu
from jax.sharding import PartitionSpec as P

discount = 0.95
lanes = 128


def gather_kernel(picks_ref, act_ref, alpha_ref, weights_ref, moves_ref, out_ref):
    beliefs = act_ref.shape[0]
    obs_local = picks_ref.shape[0] // beliefs
    actions = weights_ref.shape[0] // obs_local
    slabs = alpha_ref.shape[1]
    rows = out_ref.shape[0] // slabs

    def one(b, carry):
        action = act_ref[b]
        sums = [None] * min(4, obs_local)
        for o in range(obs_local):
            row = alpha_ref[picks_ref[b * obs_local + o]].astype(jnp.float32)
            term = row * weights_ref[o * actions + action]
            at = o % len(sums)
            sums[at] = term if sums[at] is None else sums[at] + term
        out_ref[pl.ds(b, slabs, stride=rows), :] = functools.reduce(jnp.add, sums)
        return carry

    lax.fori_loop(0, beliefs, one, 0)

    def total(a, carry):
        acc = weights_ref[a]
        for o in range(1, obs_local):
            acc = acc + weights_ref[o * actions + a]
        out_ref[pl.ds(beliefs + a, slabs, stride=rows), :] = acc
        out_ref[pl.ds(beliefs + actions + a, slabs, stride=rows), :] = moves_ref[a]
        return carry

    lax.fori_loop(0, actions, total, 0)


def gather_rows(picks, acts, alpha, weights, moves):
    slabs = alpha.shape[1]
    beliefs = acts.shape[0]
    rows = beliefs + 2 * moves.shape[0]
    vmem = pl.BlockSpec(memory_space=pltpu.VMEM)
    smem = pl.BlockSpec(memory_space=pltpu.SMEM)
    out = pl.pallas_call(
        gather_kernel,
        out_shape=jax.ShapeDtypeStruct((slabs * rows, lanes), jnp.float32),
        in_specs=[smem, smem, vmem, vmem, vmem],
        out_specs=vmem,
        compiler_params=pltpu.CompilerParams(vmem_limit_bytes=40 << 20),
        cost_estimate=pl.CostEstimate(
            flops=80_000_000, bytes_accessed=16 << 20, transcendentals=0
        ),
        name="gather_rows",
    )(picks, acts, alpha, weights, moves)
    return out.reshape(slabs, rows, lanes)


def move_kernel(act_ref, w_ref, tot_ref, table_ref, out_ref):
    a = pl.program_id(0)
    scaled = w_ref[...] / tot_ref[0]
    x = jnp.where(act_ref[...] == a, scaled, 0.0)
    high = x.astype(jnp.bfloat16)
    low = (x - high.astype(jnp.float32)).astype(jnp.bfloat16)
    table = table_ref[0]
    both = jnp.dot(jnp.concatenate([high, low], axis=0), table, preferred_element_type=jnp.float32)
    half = x.shape[0]
    part = both[:half] + both[half:]

    @pl.when(a == 0)
    def _():
        out_ref[...] = part

    @pl.when(a > 0)
    def _():
        out_ref[...] += part


def move(acts, weighted, totals, table):
    beliefs, width = weighted.shape
    actions, _, states = table.shape
    return pl.pallas_call(
        move_kernel,
        grid=(actions,),
        out_shape=jax.ShapeDtypeStruct((beliefs, states), jnp.float32),
        in_specs=[
            pl.BlockSpec((beliefs, 1), lambda a: (0, 0)),
            pl.BlockSpec((beliefs, width), lambda a: (0, 0)),
            pl.BlockSpec((1, 1, width), lambda a: (a, 0, 0)),
            pl.BlockSpec((1, width, states), lambda a: (a, 0, 0)),
        ],
        out_specs=pl.BlockSpec((beliefs, states), lambda a: (0, 0)),
        compiler_params=pltpu.CompilerParams(
            vmem_limit_bytes=48 << 20, dimension_semantics=("arbitrary",)
        ),
        cost_estimate=pl.CostEstimate(
            flops=4 * beliefs * width * actions * states,
            bytes_accessed=2 * actions * width * states,
            transcendentals=0,
        ),
        name="move",
    )(acts[:, None], weighted, totals[:, None, :], table)


def action_table(actions, count):
    return (actions[:, None] == jnp.arange(count, dtype=jnp.int32)[None, :]).astype(jnp.float32)


MESH = pl.DeviceIdType.MESH
code_top = 32767.0


def encode(values, top):
    q = (values * (code_top / top) + (code_top + 1.5)).astype(jnp.int32) - 32768
    return q.astype(jnp.int16)


def column_top(blocks):
    tops = [jnp.max(jnp.abs(v), axis=0, keepdims=True) for v in blocks]
    return jnp.maximum(functools.reduce(jnp.maximum, tops), 1e-30)


def decode(codes, scale):
    return codes.astype(jnp.int32).astype(jnp.float32) * scale


def fused_kernel(plan, names, *refs):
    r = types.SimpleNamespace(**dict(zip(names, refs)))
    ranks, groups, actions, obs_local, rows, cols, beliefs, parts_of, width = plan
    zs, ys = ranks // 2, groups // 2
    sps = cols // lanes
    slabs = zs * sps
    owned = beliefs // ranks
    half_obs = obs_local // 2
    chunk, tail = parts_of
    first_rows = ranks * chunk
    counts = (ranks, ranks * tail // chunk)
    steps = zs * 2 * cols // width
    share = steps // groups
    parts = r.a_yr.shape[2]
    part_rows = rows // parts
    pairs = zs // 2

    me_o, me_b = lax.axis_index("obs"), lax.axis_index("bel")
    z, x = lax.div(me_o, 2), lax.rem(me_o, 2)
    y, c = lax.div(me_b, 2), lax.rem(me_b, 2)
    odd = lax.rem(z, 2)
    other = me_b + 1 - 2 * c
    x_peer = {"obs": me_o + 1 - 2 * x}
    core_peer = {"bel": other}
    next_z = {"obs": (z + 1 - 2 * odd) * 2 + x}
    z_at = [lax.rem(z + d, zs) for d in range(zs)]
    z_peer = [{"obs": zt * 2 + x} for zt in z_at]
    y_peer = [{"bel": lax.rem(y + d, ys) * 2 + c} for d in range(ys)]
    y_from = [lax.rem(y + ys - d, ys) for d in range(ys)]
    b_peer = [{"bel": lax.rem(me_b + d, groups)} for d in range(groups)]
    b_from = [lax.rem(me_b + groups - d, groups) for d in range(groups)]

    def remote(src, dst, s_sem, r_sem, where):
        return pltpu.make_async_remote_copy(
            src_ref=src,
            dst_ref=dst,
            send_sem=s_sem,
            recv_sem=r_sem,
            device_id=where,
            device_id_type=MESH,
        )

    def drain_sends(ref, sem):
        remote(ref, ref, sem, sem, x_peer).wait_send()

    def drain_receives(ref, sem):
        remote(ref, ref, sem, sem, x_peer).wait_recv()

    def drain_local(ref, sem):
        pltpu.make_async_copy(ref, ref, sem).wait()

    def band(s):
        return pl.ds(pl.multiple_of(s * cols, lanes), cols)

    def source_band(s, side):
        return pl.ds(pl.multiple_of((2 * s + side) * cols, lanes), cols)

    def half(side):
        return pl.ds(side * half_obs, half_obs)

    small = [
        pltpu.make_async_copy(r.act_hbm, r.act, r.small_sem.at[0]),
        pltpu.make_async_copy(r.act_hbm, r.act_row, r.small_sem.at[1]),
        pltpu.make_async_copy(r.rew_hbm, r.rew, r.small_sem.at[2]),
    ]
    own_idx = pltpu.make_async_copy(r.idx, r.idx_in, r.idx_sem)
    peer_w = [
        pltpu.make_async_copy(
            r.weights.at[half(c), :, source_band(s, 1 - x)], r.w_src.at[s], r.loc_sem.at[s]
        )
        for s in range(zs)
    ]
    own_w = [
        pltpu.make_async_copy(
            r.weights.at[:, :, source_band(s, x)], r.wraw.at[:, :, band(s)], r.ow_sem
        )
        for s in range(zs)
    ]
    own_a = [
        pltpu.make_async_copy(
            r.alpha.at[:, source_band(s, x)], r.araw.at[me_b, :, band(s)], r.oa_sem
        )
        for s in range(zs)
    ]
    table = []
    for k in range(steps):
        n = lax.rem(me_b * share + k, steps)
        at = pl.ds(pl.multiple_of(n * width, lanes), width)
        table.append(pltpu.make_async_copy(r.trans.at[:, at], r.tvm.at[n], r.tr_sem.at[min(k, share)]))
    for copy in peer_w + [own_idx] + small + own_w + table[:share] + own_a + table[share:]:
        copy.start()

    peers = [x_peer] + z_peer[1:] + b_peer[1:]
    barrier = pltpu.get_barrier_semaphore()
    for peer in peers:
        pl.semaphore_signal(barrier, inc=1, device_id=peer, device_id_type=MESH)
    pl.semaphore_wait(barrier, len(peers))

    def rows_of(h):
        return pl.ds(h * part_rows, part_rows)

    def near(k):
        return 2 * k + odd

    def far(k):
        return 2 * k + 1 - odd

    pieces = [(k, h) for k in range(pairs) for h in range(parts)]
    def launch(copy):
        copy.start()

    for k, h in pieces:
        for d in range(1, ys):
            launch(
                remote(
                    r.alpha.at[rows_of(h), source_band(near(k), x)],
                    r.araw.at[me_b, rows_of(h), band(near(k))],
                    r.a_ys.at[d - 1],
                    r.a_yr.at[d - 1, k, h],
                    y_peer[d],
                )
            )
    a_core = [
        remote(
            r.alpha.at[:, source_band(s, x)],
            r.araw.at[me_b, :, band(s)],
            r.a_ps,
            r.a_pr,
            core_peer,
        )
        for s in range(zs)
    ]
    for copy in a_core:
        launch(copy)

    w_out = []
    for s in range(zs):
        peer_w[s].wait()
        for at in range(0, cols, lanes):
            value = r.w_src[s, :, :, at : at + lanes]
            top = jnp.maximum(jnp.max(jnp.abs(value), axis=0), 1e-30)
            r.w_code_s[s, :, :, at : at + lanes] = encode(value, top[None])
            r.w_scale_s[s, :, at : at + lanes] = top * (1.0 / code_top)
        w_out.append(
            (
                remote(r.w_code_s.at[s], r.w_code.at[c, s], r.w_xs.at[0], r.w_xr.at[0, s], x_peer),
                remote(
                    r.w_scale_s.at[s], r.w_scale.at[c, s], r.w_xs.at[1], r.w_xr.at[1, s], x_peer
                ),
            )
        )
        for copy in w_out[-1]:
            launch(copy)

    pick_sm = [getattr(r, f"pick_{k}") for k in range(2 * obs_local)]

    def store_picks(source, first):
        for o in range(obs_local):
            pltpu.make_async_copy(
                source.at[pl.ds(o, 1), :], pick_sm[first + o], r.pk_l.at[first // obs_local]
            ).start()

    def own_picks():
        for copy in small + [own_idx]:
            copy.wait()
        action_row = r.act_row[...].reshape(1, beliefs)
        chosen = jnp.zeros((obs_local, beliefs), jnp.int32)
        for a in range(actions):
            chosen = jnp.where(action_row == a, r.idx_in[a], chosen)
        r.pick_out[...] = chosen * slabs

    pick_copy = remote(r.pick_out, r.pick_in, r.pk_s, r.pk_r, x_peer)
    tt_out = [
        remote(r.tpart, r.tz.at[d - 1], r.tt_zs, r.tt_zr, z_peer[d])
        for d in range(1, zs)
    ]
    tx_out = remote(r.tx.at[0], r.tx.at[1], r.tt_xs, r.tt_xr, x_peer)

    def transition_totals():
        for k in range(share):
            table[k].wait()
            n = me_b * share + k

            def column_total(a, carry, n=n, k=k):
                value = r.tvm[n, pl.ds(pl.multiple_of(a * cols, 16), cols), :].astype(jnp.float32)
                r.tpart[pl.ds(a, 1), k * width : (k + 1) * width] = jnp.sum(
                    value, axis=0, keepdims=True
                )
                return carry

            lax.fori_loop(0, actions, column_total, 0)

    def action_lanes(owner, carry):
        for k in range(owned):
            at = owner * chunk + k if k < chunk else first_rows + owner * tail + k - chunk
            r.actb[pl.ds(at, 1), :] = jnp.full((1, lanes), r.act[owner * owned + k], jnp.int32)
        return carry

    pad = slabs

    def own_weight_slab(s):
        def one(o, carry):
            for h in range(sps):
                at = s * cols + h * lanes
                first = o * actions * slabs + s * sps + h + pad
                r.wslab[pl.ds(first, actions, stride=slabs), :] = r.wraw[o, :, at : at + lanes]
            return carry

        lax.fori_loop(0, obs_local, one, 0)

    def peer_weight_slab(side, s):
        def one(o, carry):
            for h in range(sps):
                at = slice(h * lanes, (h + 1) * lanes)
                first = (obs_local + side * half_obs + o) * actions * slabs + s * sps + h + pad
                r.wslab[pl.ds(first, actions, stride=slabs), :] = decode(
                    r.w_code[side, s, o, :, at], r.w_scale[side, s, :, at]
                )
            return carry

        lax.fori_loop(0, half_obs, one, 0)

    def alpha_slab(member, s, first_row, count):
        def one(i, carry):
            for k in range(2):
                r0 = pl.multiple_of(first_row + i * 32 + k * 16, 16)
                for h in range(sps):
                    at = pl.ds(pl.multiple_of(s * cols + h * lanes, lanes), lanes)
                    first = (member * rows + r0) * slabs + s * sps + h
                    r.aslab[pl.ds(first, 16, stride=slabs), :] = r.araw[
                        member, pl.ds(r0, 16), at
                    ].astype(jnp.float32)
            return carry

        lax.fori_loop(0, count // 32, one, 0)

    late = []

    def arrived(k, h, by_z):
        s = far(k) if by_z else near(k)
        for d in range(1, ys):
            member = y_from[d] * 2 + c
            slot = r.araw.at[member, rows_of(h), band(s)]
            here = (d - 1, k, h)
            if by_z:
                drain_receives(slot, r.a_zr.at[here])
            else:
                drain_receives(slot, r.a_yr.at[here])
                launch(remote(slot, slot, r.a_zs.at[d - 1], r.a_zr.at[here], next_z))
            at = (d - 1, int(by_z), k, h)
            forward = remote(slot, slot, r.a_fs.at[d - 1], r.a_fr.at[at], core_peer)
            launch(forward)
            alpha_slab(member, s, h * part_rows, part_rows)

            def rest(forward=forward, member=y_from[d] * 2 + 1 - c):
                forward.wait_recv()
                alpha_slab(member, s, h * part_rows, part_rows)

            late.append(rest)

    def weights_arrived(s):
        both = []
        for k, copy in enumerate(w_out[s]):
            copy.wait_recv()
            held = (r.w_code, r.w_scale)[k].at[c, s]
            both.append(remote(held, held, r.w_fs.at[k], r.w_fr.at[k, s], core_peer))
            launch(both[-1])
        peer_weight_slab(c, s)

        def rest():
            for copy in both:
                copy.wait_recv()
            peer_weight_slab(1 - c, s)

        late.append(rest)

    own_picks()
    pick_copy.start()
    store_picks(r.pick_out, 0)
    drain_local(r.wraw, r.ow_sem)
    for s in range(zs):
        own_weight_slab(s)
    drain_local(r.araw.at[me_b], r.oa_sem)
    for s in range(zs):
        alpha_slab(me_b, s, 0, rows)
    lax.fori_loop(0, ranks, action_lanes, 0)
    count = len(pieces)
    for i in range(count + 1):
        ready, late = late, []
        if i < count:
            arrived(*pieces[i], False)
        if i >= 1:
            arrived(*pieces[i - 1], True)
        for s in range(i * zs // (count + 1), (i + 1) * zs // (count + 1)):
            weights_arrived(s)
        for rest in ready:
            rest()
        if i == 0:
            transition_totals()
            for copy in tt_out:
                copy.start()
        if i == 1:
            drain_receives(r.araw.at[other], r.a_pr)
            for s in range(zs):
                alpha_slab(other, s, 0, rows)
        if i == 2:
            pick_copy.wait()
            store_picks(r.pick_in, obs_local)
    for rest in late:
        rest()
    drain_sends(r.tz, r.tt_zs)
    drain_receives(r.tz, r.tt_zr)
    total = r.tpart[...]
    for d in range(1, zs):
        total = total + r.tz[d - 1]
    r.tx[0] = total

    def obs_total(a, carry):
        sums = [None] * 4
        for o in range(2 * obs_local):
            term = r.wslab[pl.ds(pl.multiple_of((o * actions + a) * slabs + pad, slabs), slabs), :]
            sums[o % 4] = term if sums[o % 4] is None else sums[o % 4] + term
        r.totst[pl.ds(a, slabs, stride=actions), :] = (sums[0] + sums[1]) + (sums[2] + sums[3])
        return carry

    lax.fori_loop(0, actions, obs_total, 0)
    tot_rows = sps * actions
    tot_out = [
        remote(
            r.totst.at[pl.ds(pl.multiple_of(z_at[d] * tot_rows, 8), tot_rows)],
            r.totrv.at[d - 1],
            r.tot_s,
            r.tot_r,
            z_peer[d],
        )
        for d in range(1, zs)
    ]
    tall_out = [
        remote(
            r.tall.at[me_b], r.tall.at[me_b], r.tall_s, r.tall_r, b_peer[d]
        )
        for d in range(1, groups)
    ]
    for copy in tot_out + [tx_out]:
        copy.start()
    drain_local(r.pick_out, r.pk_l.at[0])
    drain_local(r.pick_in, r.pk_l.at[1])

    def share_totals():
        tx_out.wait()
        r.tall[me_b] = r.tx[0] + r.tx[1]
        for copy in tall_out:
            copy.start()

    def p_copies(q, d):
        here = (q, d - 1)
        return (
            remote(r.psend.at[here], r.precv.at[here], r.p_s, r.p_r.at[q], z_peer[d]),
            remote(
                r.pscale_s.at[here], r.pscale_r.at[here], r.ps_s, r.ps_r.at[q], z_peer[d]
            ),
        )

    unroll = 4

    def gather_chunk(q, part):
        def one(i, carry):
            if part == 0:
                b0 = q * owned + i * unroll
            else:
                row = i * unroll
                owner = (q - ranks) * (chunk // tail) + lax.div(row, tail)
                b0 = owner * owned + chunk + lax.rem(row, tail)
            for t in range(unroll):
                b = b0 + t
                base = r.act[b] * slabs
                sums = [None] * 4
                for p in range(2):
                    for o in range(obs_local):
                        row = r.aslab[pl.ds(pick_sm[p * obs_local + o][0, b], slabs), :]
                        at = (p * obs_local + o) * actions * slabs + pad
                        term = row * r.wslab[pl.ds(base + at, slabs), :]
                        k = o % 4
                        sums[k] = term if sums[k] is None else sums[k] + term
                r.stage[pl.ds(q * chunk + i * unroll + t, slabs, stride=beliefs), :] = (sums[0] + sums[1]) + (
                    sums[2] + sums[3]
                )
            return carry

        lax.fori_loop(0, chunk // unroll, one, 0)
        for d in range(1, zs):
            for h in range(sps):
                first = (z_at[d] * sps + h) * beliefs + q * chunk
                value = r.stage[pl.ds(pl.multiple_of(first, 8), chunk), :]
                top = column_top([value])
                r.psend[q, d - 1, h] = encode(value, top)
                r.pscale_s[q, d - 1, h : h + 1, :] = top * (1.0 / code_top)
            for copy in p_copies(q, d):
                copy.start()

    def prepare():
        drain_sends(r.totrv, r.tot_s)
        drain_receives(r.totrv, r.tot_r)
        totals = r.totst[pl.ds(pl.multiple_of(z * tot_rows, 8), tot_rows), :]
        for d in range(1, zs):
            totals = totals + r.totrv[d - 1]
        r.tsum[...] = totals

    def own_rows():
        drain_sends(r.tall.at[pl.ds(0, groups - 1)], r.tall_s)
        drain_receives(r.tall.at[pl.ds(0, groups - 1)], r.tall_r)
        own_act = jnp.concatenate(
            [
                r.actb[pl.ds(pl.multiple_of(me_o * chunk, 8), chunk), :],
                r.actb[pl.ds(pl.multiple_of(first_rows + me_o * tail, 8), tail), :],
            ],
            axis=0,
        )
        per_member = share * width // lanes

        for member in range(groups):
            for k in range(per_member):
                at = slice(k * lanes, (k + 1) * lanes)
                to = slice((member * per_member + k) * lanes, (member * per_member + k + 1) * lanes)
                reward = jnp.zeros((owned, lanes), jnp.float32)
                scale = jnp.ones((owned, lanes), jnp.float32)
                for a in range(actions):
                    hit = own_act == a
                    reward = jnp.where(hit, r.rew[a : a + 1, to], reward)
                    scale = jnp.where(hit, r.tall[member, a : a + 1, at], scale)
                r.rsel[:, to] = reward
                r.tsel[:, to] = discount / scale

    def absorb(q, part):
        drain_receives(r.precv.at[q], r.p_r.at[q])
        drain_receives(r.pscale_r.at[q], r.ps_r.at[q])
        b0 = pl.multiple_of(q * chunk, 16)
        into = (r.xbig0, r.xbig1)[part]
        at_row = pl.multiple_of(q * chunk - part * first_rows, 16)
        at_low = pl.multiple_of(at_row + into.shape[0] // 2, 16)
        act = r.actb[pl.ds(b0, chunk), :]
        for h in range(sps):
            first = (z * sps + h) * beliefs + q * chunk
            value = r.stage[pl.ds(pl.multiple_of(first, 8), chunk), :]
            for d in range(1, zs):
                value = value + decode(r.precv[q, d - 1, h], r.pscale_r[q, d - 1, h : h + 1, :])
            under = jnp.ones_like(value)
            for a in range(actions):
                at = h * actions + a
                under = jnp.where(act == a, r.tsum[at : at + 1, :], under)
            value = value / under
            high = value.astype(jnp.bfloat16).astype(jnp.float32)
            low = value - high
            for a in range(actions):
                at = slice(a * cols + h * lanes, a * cols + (h + 1) * lanes)
                hit = act == a
                into[pl.ds(at_row, chunk), at] = jnp.where(hit, high, 0.0).astype(jnp.bfloat16)
                into[pl.ds(at_low, chunk), at] = jnp.where(hit, low, 0.0).astype(jnp.bfloat16)

    behind = 3

    def gather_first(q, carry):
        gather_chunk(q, 0)

        @pl.when(q == 0)
        def _():
            share_totals()

        @pl.when(q == behind - 1)
        def _():
            prepare()

        @pl.when(q >= behind)
        def _():
            absorb(q - behind, 0)

        return carry

    def gather_last(j, carry):
        gather_chunk(ranks + j, 1)

        @pl.when(j < behind)
        def _():
            absorb(ranks - behind + j, 0)

        @pl.when(j == counts[1] - 1)
        def _():
            own_rows()

        return carry

    lax.fori_loop(0, counts[0], gather_first, 0)
    lax.fori_loop(0, counts[1], gather_last, 0)
    drain_local(r.tvm.at[pl.ds(0, steps - share)], r.tr_sem.at[share])

    sizes = (chunk, tail)
    sets = [
        types.SimpleNamespace(
            **{name: getattr(r, name + str(part)) for name in part_names}, rows=sizes[part]
        )
        for part in range(2)
    ]

    def x_copies(part, n):
        t, here = sets[part], (part, n)
        return (
            remote(t.xsend.at[n], t.xrecv.at[n], r.x_s.at[part], r.x_r.at[here], x_peer),
            remote(t.xscale_s.at[n], t.xscale_r.at[n], r.xs_s.at[part], r.xs_r.at[here], x_peer),
        )

    def z_copies(part, n, d):
        t, here, k = sets[part], (part, n), (n, d - 1)
        return (
            remote(t.zsend.at[k], t.zrecv.at[k], r.z_s.at[part], r.z_r.at[here], z_peer[d]),
            remote(
                t.zscale_s.at[k], t.zscale_r.at[k], r.zs_s.at[part], r.zs_r.at[here], z_peer[d]
            ),
        )

    def product(part, n):
        t = sets[part]
        both = jnp.dot(t.xbig[...], r.tvm[n], preferred_element_type=jnp.float32)
        count = both.shape[0] // 2
        t.outp[n] = both[:count] + both[count:]
        owner = [
            t.outp[n, pl.ds(pl.multiple_of((2 * s + 1 - x) * t.rows, 8), t.rows), :]
            for s in range(zs)
        ]
        top = column_top(owner)
        for s in range(zs):
            t.xsend[n, s * t.rows : (s + 1) * t.rows, :] = encode(owner[s], top)
        t.xscale_s[n] = top * (1.0 / code_top)
        for copy in x_copies(part, n):
            copy.start()

    def to_owners(part, n):
        t = sets[part]
        for copy in x_copies(part, n):
            copy.wait_recv()
        scale = t.xscale_r[n]
        for s in range(zs):
            at = slice(s * t.rows, (s + 1) * t.rows)
            kept = t.outp[n, pl.ds(pl.multiple_of((2 * s + x) * t.rows, 8), t.rows), :]
            t.ysum[n, at, :] = kept + decode(t.xrecv[n, at, :], scale)
        for d in range(1, zs):
            value = t.ysum[n, pl.ds(pl.multiple_of(z_at[d] * t.rows, 8), t.rows), :]
            top = column_top([value])
            t.zsend[n, d - 1] = encode(value, top)
            t.zscale_s[n, d - 1] = top * (1.0 / code_top)
            for copy in z_copies(part, n, d):
                copy.start()

    def finish(part, n):
        t = sets[part]
        value = t.ysum[n, pl.ds(pl.multiple_of(z * t.rows, 8), t.rows), :]
        drain_receives(t.zrecv.at[n], r.z_r.at[part, n])
        drain_receives(t.zscale_r.at[n], r.zs_r.at[part, n])
        for d in range(1, zs):
            value = value + decode(t.zrecv[n, d - 1], t.zscale_r[n, d - 1])
        at = pl.ds(pl.multiple_of(n * width, width), width)
        to = slice(part * chunk, part * chunk + t.rows)
        r.out[to, at] = r.rsel[to, at] + value * r.tsel[to, at]

    lag = min(3, steps)

    def first_step(n, carry):
        product(0, n)

        @pl.when(n >= lag)
        def _():
            to_owners(0, n - lag)

        @pl.when(n >= steps - counts[1])
        def _():
            absorb(ranks + n - (steps - counts[1]), 1)

        return carry

    def last_step(n, carry):
        product(1, n)

        @pl.when(n < lag)
        def _():
            to_owners(0, n + steps - lag)

        @pl.when(n >= lag)
        def _():
            to_owners(1, n - lag)

        finish(0, n)
        return carry

    lax.fori_loop(0, steps, first_step, 0)
    lax.fori_loop(0, steps, last_step, 0)
    for n in range(steps - lag, steps):
        to_owners(1, n)
    for n in range(steps):
        finish(1, n)
    for part, t in enumerate(sets):
        drain_sends(t.xsend, r.x_s.at[part])
        drain_sends(t.xscale_s, r.xs_s.at[part])
        drain_sends(t.zsend, r.z_s.at[part])
        drain_sends(t.zscale_s, r.zs_s.at[part])
    drain_sends(r.psend, r.p_s)
    drain_sends(r.pscale_s, r.ps_s)
    drain_sends(r.w_code_s, r.w_xs.at[0])
    drain_sends(r.w_scale_s, r.w_xs.at[1])
    drain_sends(r.w_code.at[0], r.w_fs.at[0])
    drain_sends(r.w_scale.at[0], r.w_fs.at[1])
    drain_sends(r.araw.at[0], r.a_ps)
    for d in range(1, ys):
        drain_sends(r.araw.at[0, :, pl.ds(0, pairs * cols)], r.a_ys.at[d - 1])
        drain_sends(r.araw.at[0, :, pl.ds(0, pairs * cols)], r.a_zs.at[d - 1])
        drain_sends(r.araw.at[0], r.a_fs.at[d - 1])


part_names = (
    "xbig",
    "outp",
    "ysum",
    "xsend",
    "xrecv",
    "xscale_s",
    "xscale_r",
    "zsend",
    "zrecv",
    "zscale_s",
    "zscale_r",
)


def fused(alpha_set, transitions, obs_weights, rewards, chosen_idx, chosen_action, groups):
    actions, states = rewards.shape
    obs_local = obs_weights.shape[0]
    beliefs = chosen_action.shape[0]
    ranks = lax.axis_size("obs")
    rows = alpha_set.shape[0]
    cols = states // ranks
    zs, ys = ranks // 2, groups // 2
    sps = cols // lanes
    slabs = zs * sps
    owned = beliefs // ranks
    half_obs = obs_local // 2
    tail = 16
    chunk = owned - tail
    chunks = ranks + ranks * tail // chunk
    width = 256
    steps = states // width
    xc = zs * cols
    shared = states // groups
    outer, parts, pairs = max(ys - 1, 1), 2, zs // 2
    plan = (ranks, groups, actions, obs_local, rows, cols, beliefs, (chunk, tail), width)
    f32, bf16, i16, i32 = jnp.float32, jnp.bfloat16, jnp.int16, jnp.int32
    vmem, dma = pltpu.VMEM, pltpu.SemaphoreType.DMA
    scratch = dict(
        act=pltpu.SMEM((beliefs,), i32),
        act_row=vmem((beliefs,), i32),
        rew=vmem((actions, states), f32),
        small_sem=dma((3,)),
        idx_in=vmem((actions, obs_local, beliefs), i32),
        araw=vmem((groups, rows, xc), bf16),
        aslab=vmem((groups * rows * slabs, lanes), f32),
        wraw=vmem((obs_local, actions, xc), f32),
        w_src=vmem((zs, half_obs, actions, cols), f32),
        w_code_s=vmem((zs, half_obs, actions, cols), i16),
        w_scale_s=vmem((zs, actions, cols), f32),
        w_code=vmem((2, zs, half_obs, actions, cols), i16),
        w_scale=vmem((2, zs, actions, cols), f32),
        wslab=vmem(((2 * obs_local * actions + 1) * slabs, lanes), f32),
        tvm=vmem((steps, actions * cols, width), bf16),
        pick_out=vmem((obs_local, beliefs), i32),
        pick_in=vmem((obs_local, beliefs), i32),
        actb=vmem((beliefs, lanes), i32),
        stage=vmem((slabs * beliefs, lanes), f32),
        totst=vmem((slabs * actions, lanes), f32),
        totrv=vmem((zs - 1, sps * actions, lanes), f32),
        tsum=vmem((sps * actions, lanes), f32),
        psend=vmem((chunks, zs - 1, sps, chunk, lanes), i16),
        precv=vmem((chunks, zs - 1, sps, chunk, lanes), i16),
        pscale_s=vmem((chunks, zs - 1, sps, lanes), f32),
        pscale_r=vmem((chunks, zs - 1, sps, lanes), f32),
        tpart=vmem((actions, shared), f32),
        tz=vmem((zs - 1, actions, shared), f32),
        tx=vmem((2, actions, shared), f32),
        tall=vmem((groups, actions, shared), f32),
        rsel=vmem((owned, states), f32),
        tsel=vmem((owned, states), f32),
        **{f"pick_{k}": pltpu.SMEM((1, beliefs), i32) for k in range(2 * obs_local)},
        pk_l=dma((2,)),
        idx_sem=dma(()),
        ow_sem=dma(()),
        oa_sem=dma(()),
        loc_sem=dma((zs,)),
        tr_sem=dma((steps // groups + 1,)),
        a_ys=dma((outer,)),
        a_yr=dma((outer, pairs, parts)),
        a_zs=dma((outer,)),
        a_zr=dma((outer, pairs, parts)),
        a_fs=dma((outer,)),
        a_fr=dma((outer, 2, pairs, parts)),
        a_ps=dma(()),
        a_pr=dma(()),
        w_xs=dma((2,)),
        w_xr=dma((2, zs)),
        w_fs=dma((2,)),
        w_fr=dma((2, zs)),
        pk_s=dma(()),
        pk_r=dma(()),
        tt_zs=dma(()),
        tt_zr=dma(()),
        tt_xs=dma(()),
        tt_xr=dma(()),
        tall_s=dma(()),
        tall_r=dma(()),
        tot_s=dma(()),
        tot_r=dma(()),
        p_s=dma(()),
        p_r=dma((chunks,)),
        ps_s=dma(()),
        ps_r=dma((chunks,)),
        x_s=dma((2,)),
        x_r=dma((2, steps)),
        xs_s=dma((2,)),
        xs_r=dma((2, steps)),
        z_s=dma((2,)),
        z_r=dma((2, steps)),
        zs_s=dma((2,)),
        zs_r=dma((2, steps)),
    )
    for part, count in enumerate((chunk, tail)):
        shapes = (
            vmem((2 * ranks * count, actions * cols), bf16),
            vmem((steps, ranks * count, width), f32),
            vmem((steps, zs * count, width), f32),
            vmem((steps, zs * count, width), i16),
            vmem((steps, zs * count, width), i16),
            vmem((steps, 1, width), f32),
            vmem((steps, 1, width), f32),
            vmem((steps, zs - 1, count, width), i16),
            vmem((steps, zs - 1, count, width), i16),
            vmem((steps, zs - 1, 1, width), f32),
            vmem((steps, zs - 1, 1, width), f32),
        )
        scratch.update(zip([name + str(part) for name in part_names], shapes))
    hbm = pl.BlockSpec(memory_space=pl.ANY)
    local = pl.BlockSpec(memory_space=pltpu.VMEM)
    names = ("act_hbm", "rew_hbm", "idx", "alpha", "weights", "trans", "out", *scratch)
    return pl.pallas_call(
        functools.partial(fused_kernel, plan, names),
        out_shape=jax.ShapeDtypeStruct((owned, states), f32),
        in_specs=[hbm] * 6,
        out_specs=local,
        scratch_shapes=list(scratch.values()),
        compiler_params=pltpu.CompilerParams(
            collective_id=0, has_side_effects=True, vmem_limit_bytes=67043328
        ),
        name="backup",
    )(
        chosen_action,
        rewards,
        chosen_idx.transpose(1, 2, 0),
        alpha_set,
        obs_weights,
        transitions.reshape(actions * cols, states),
    )


def fits(alpha_set, transitions, obs_weights, beliefs, ranks, groups):
    cols = transitions.shape[1]
    obs_local, actions, states = obs_weights.shape
    return (
        ranks % 4 == 0
        and groups % 2 == 0
        and cols % lanes == 0
        and states == ranks * cols
        and states % (256 * groups) == 0
        and actions % 8 == 0
        and obs_local % 2 == 0
        and alpha_set.shape[0] % 64 == 0
        and beliefs % (16 * ranks) == 0
        and beliefs > 16 * ranks
        and ranks * 16 % (beliefs // ranks - 16) == 0
        and ranks * 16 // (beliefs // ranks - 16) <= states // 256
        and ranks * 16 // (beliefs // ranks - 16) >= 3
    )


def body(alpha_set, transitions, obs_weights, rewards, chosen_idx, chosen_action):
    actions, states = rewards.shape
    obs_local = obs_weights.shape[0]
    beliefs = chosen_action.shape[0]
    slabs = states // lanes
    ranks = lax.axis_size("obs")
    groups = lax.axis_size("bel")
    if fits(alpha_set, transitions, obs_weights, beliefs, ranks, groups):
        return fused(
            alpha_set, transitions, obs_weights, rewards, chosen_idx, chosen_action, groups
        )
    action_hot = action_table(chosen_action, actions)
    picks = jnp.sum(jnp.where(action_hot[:, :, None] > 0, chosen_idx, 0), axis=1).reshape(-1)
    alpha = lax.all_gather(alpha_set.reshape(-1, slabs, lanes), "bel", axis=0, tiled=True)
    weights = obs_weights.reshape(obs_local * actions, slabs, lanes)
    trans_part = jnp.sum(transitions.astype(jnp.float32), axis=1).reshape(actions, slabs, lanes)
    partial = gather_rows(picks, chosen_action, alpha, weights, trans_part)
    rows = partial.shape[1]
    if slabs % ranks == 0:
        piece = lax.psum_scatter(partial, "obs", scatter_dimension=0, tiled=True)
        piece = piece.transpose(1, 0, 2).reshape(rows, -1)
    else:
        flat = partial.transpose(1, 0, 2).reshape(rows, states)
        piece = lax.psum_scatter(flat, "obs", scatter_dimension=1, tiled=True)
    trans_totals = lax.all_gather(piece[beliefs + actions :], "obs", axis=1, tiled=True)
    moved = move(
        chosen_action, piece[:beliefs], piece[beliefs : beliefs + actions], transitions
    )
    future = lax.psum_scatter(moved, "obs", scatter_dimension=0, tiled=True)
    owned = beliefs // ranks
    own_hot = lax.dynamic_slice_in_dim(action_hot, lax.axis_index("obs") * owned, owned, 0)
    own = functools.partial(
        jnp.dot, own_hot, precision=lax.Precision.HIGHEST, preferred_element_type=jnp.float32
    )
    return own(rewards) + discount * (future / own(trans_totals))


def solution(mesh):
    placed = (
        P("bel", None),
        P(None, "obs", None),
        P("obs", None, None),
        P(),
        P("bel", None, "obs"),
        P("bel"),
    )
    return jax.shard_map(
        body, mesh=mesh, in_specs=placed, out_specs=P(("bel", "obs"), None), check_vma=False
    )
```
